128 devices in a mesh: ctx: 8 (over z_lo, y), tp: 16 (over z_hi, x, core).
Axes of the slice: x: 4, y: 4, z: 4 (z_hi: 2, z_lo: 2; z = z_hi * 2 + z_lo), core: 2. Of those that a mesh axis runs over, the one named last changes fastest.
Arguments:
- queries: bfloat16 [8192, 8192], P('ctx', 'tp'), may hold values from -64 to 64
- context_keys: bfloat16 [8192, 1024], P('ctx'), may hold values from -6 to 6
- context_values: bfloat16 [8192, 1024], P('ctx'), may hold values from -6 to 6
- positions: int32 [8192], P('ctx'), may hold values from 0 to 8191, as said below
- out_weight: bfloat16 [8192, 8192], P('tp'), may hold values from -0.5 to 0.5
- residual_in: bfloat16 [8192, 8192], P(('ctx', 'tp')), may hold values from -3 to 3
- norm_gain: float32 [8192], replicated, may hold values from 0.5 to 1.5
- static_scale: float32 [1], replicated, may hold values from 0.004 to 0.009
Outputs:
- hidden_out: bfloat16 [8192, 8192], P(('ctx', 'tp'))
- clipped: bfloat16 [8192, 8192], P(('ctx', 'tp'))
The draws below stay inside these ranges and needn't reach their ends.
Inputs may be any that keep to these rules, and one draw needn't show every extreme that they name: Rows fall into aligned runs of 512 rows that hold consecutive positions in increasing order; all positions together are a permutation of 0 to 8191.
All inputs are finite; a program needn't handle non-finite values.
Results may differ from the reference program's by a relative error of at most 0.017.
Values may be sent and summed in bfloat16 or wider, within the bound.
No kernel may reach another device: no remote copies, remote signals or barrier semaphores. Data moves between devices by JAX's collectives and lax.ppermute only.
A program may use at most 128 MiB of HBM per device.

```python
import math
import jax
import jax.numpy as jnp
from jax import lax

D = 8192
HEADS = 64
KVH = 8
HD = 128
TOK_DEV = 1024
SPAN = 512
TOKENS = 8192
N_TP = 16


def span_order(key):
    return jax.random.permutation(jax.random.fold_in(key, 5), TOKENS // SPAN).astype(jnp.int32)


def row_positions(key):
    order = span_order(key)
    row_ids = jnp.arange(TOKENS, dtype=jnp.int32)
    return (order[row_ids // SPAN] * SPAN + row_ids % SPAN).astype(jnp.int32)


def shared_draw(key):
    base_key = jax.random.fold_in(key, 71)
    first_key, second_key = jax.random.split(base_key, 2)
    key_table = jnp.clip(jax.random.normal(first_key, (TOKENS, KVH * HD), jnp.float32), -6.0, 6.0)
    query_table = jnp.clip(1.5 * jax.random.normal(second_key, (TOKENS, HEADS * HD), jnp.float32), -9.0, 9.0)
    return (query_table, key_table)


def draw_queries(key, part):
    return shared_draw(key)[0].astype(jnp.bfloat16)


def draw_context_keys(key, part):
    return shared_draw(key)[1].astype(jnp.bfloat16)


def draw_positions(key, part):
    return row_positions(key)


def shard_levels(stream_key, dims, pieces, least, high):
    level = 1.0
    for dim, shards_of in pieces:
        steps = jax.random.uniform(jax.random.fold_in(jax.random.fold_in(stream_key, 6), dim), (shards_of,), jnp.float32, least / len(pieces), high / len(pieces))
        level = level * jnp.repeat(jnp.exp(steps), dims[dim] // shards_of).reshape((-1,) + (1,) * (len(dims) - 1 - dim))
    return level


def scatter_about(stream_key, shape, spread, most, pieces=(), kind=jnp.bfloat16):
    level = shard_levels(stream_key, shape, pieces, -0.22, 0.18) if pieces else 1.0
    entries = jax.random.normal(stream_key, shape, jnp.float32) * spread * level
    return jnp.minimum(jnp.maximum(entries, -most), most).astype(kind)


def setup_inputs(seed: int = 0) -> dict:
    key_of = jax.random.split(jax.random.key(seed), 9)
    queries = draw_queries(jax.random.fold_in(key_of[8], 71), 0)
    context_keys = draw_context_keys(jax.random.fold_in(key_of[8], 71), 0)
    context_values = scatter_about(key_of[2], (TOKENS, KVH * HD), 1.0, 6.0, ((0, 8),))
    positions = draw_positions(jax.random.fold_in(key_of[8], 71), 0)
    out_weight = scatter_about(key_of[4], (HEADS * HD, D), HD ** -0.5, 0.5, ((0, 16),))
    residual_in = scatter_about(key_of[5], (TOKENS, D), 0.5, 3.0, ((0, 128),))
    norm_gain = jnp.clip(1.0 + 0.1 * jax.random.normal(key_of[6], (D,), jnp.float32), 0.5, 1.5)
    static_scale = jnp.clip(jnp.exp(jax.random.uniform(key_of[7], (1,), jnp.float32, math.log(0.004), math.log(0.009))), 0.004, 0.009)
    return dict(queries=queries, context_keys=context_keys, context_values=context_values, positions=positions, out_weight=out_weight, residual_in=residual_in, norm_gain=norm_gain, static_scale=static_scale)


masked_fill = -1e+30

def attend_head(head, queries, context_keys, context_values, positions):
    kv_head = head // (HEADS // KVH)
    query_cols = lax.dynamic_slice_in_dim(queries, head * HD, HD, 1).astype(jnp.float32)
    key_cols = lax.dynamic_slice_in_dim(context_keys, kv_head * HD, HD, 1).astype(jnp.float32)
    value_cols = lax.dynamic_slice_in_dim(context_values, kv_head * HD, HD, 1).astype(jnp.float32)
    block_count = TOKENS // TOK_DEV

    def one_block(block_args):
        query_blk, query_pos = block_args
        scores = jnp.dot(query_blk, key_cols.T, preferred_element_type=jnp.float32, precision=lax.Precision.HIGHEST) * (1.0 / math.sqrt(HD))
        allowed = positions[None, :] <= query_pos[:, None]
        row_max = lax.optimization_barrier(jnp.max(jnp.where(allowed, scores, masked_fill), axis=1))
        expo = jnp.where(allowed, jnp.exp(scores - row_max[:, None]), 0.0)
        row_total = lax.optimization_barrier(jnp.sum(expo, axis=1))
        rounded = lax.optimization_barrier(expo.astype(jnp.bfloat16))
        output = jnp.dot(rounded.astype(jnp.float32), value_cols, preferred_element_type=jnp.float32, precision=lax.Precision.HIGHEST)
        return (output / row_total[:, None]).astype(jnp.bfloat16)
    finished = lax.map(one_block, (query_cols.reshape(block_count, TOK_DEV, HD), positions.reshape(block_count, TOK_DEV)))
    return finished.reshape(TOKENS, HD)

def reference(queries, context_keys, context_values, positions, out_weight, residual_in, norm_gain, static_scale):
    head_ids = jnp.arange(HEADS, dtype=jnp.int32)
    attended = lax.map(lambda head: attend_head(head, queries, context_keys, context_values, positions), head_ids)
    attended = jnp.transpose(attended, (1, 0, 2)).reshape(TOKENS, HEADS * HD)
    group_width = HEADS * HD // N_TP
    summed = residual_in.astype(jnp.float32)
    for group_index in range(N_TP):
        low_col = group_index * group_width
        group_term = jnp.dot(attended[:, low_col:low_col + group_width].astype(jnp.float32), out_weight[low_col:low_col + group_width].astype(jnp.float32), preferred_element_type=jnp.float32, precision=lax.Precision.HIGHEST)
        group_term = lax.optimization_barrier(group_term.astype(jnp.bfloat16))
        summed = summed + group_term.astype(jnp.float32)
    hidden_out = summed.astype(jnp.bfloat16)
    inv_rms = lax.rsqrt(lax.optimization_barrier(jnp.mean(summed * summed, axis=1, keepdims=True)) + 1e-05)
    limit = 448.0 * static_scale[0]
    clipped = jnp.clip(summed * inv_rms * norm_gain[None, :], -limit, limit).astype(jnp.bfloat16)
    return (hidden_out, clipped)
```

```python
import functools
import math

import jax
import jax.numpy as jnp
from jax import lax
from jax.experimental import pallas as pl
from jax.experimental.pallas import tpu as pltpu
from jax.sharding import PartitionSpec as P

HD = 128
SPAN = 512
GW = 256
MASKED = -1e30
LOG2_SCALE = math.log2(math.e) / math.sqrt(HD)
PARTS = 2
Y_COUNT = 4
X_COUNT = 4
ANY = pl.ANY


def attend_kernel(
    own_ref, loc_ref, core_ref, q_ref, first_ref, second_ref, out_ref,
    k_ref, v_ref, vt_ref, qt_ref, acc_ref, max_ref, sum_ref, top_ref, sems, *score_refs,
    rows, part, heads, run,
):
    span = pl.program_id(0)
    slots = first_ref.shape[0]
    block_rows = k_ref.shape[0] // slots
    nrow = q_ref.shape[0] * rows
    groups = nrow * heads // GW

    @pl.when(span == 0)
    def _():
        def fetch(k_src, v_src):
            copies = []
            for s in range(slots):
                dst = pl.ds(s * block_rows, block_rows)
                copies.append(pltpu.make_async_copy(k_src.at[s, pl.ds(0, block_rows)], k_ref.at[dst], sems.at[s]))
                copies.append(pltpu.make_async_copy(v_src.at[s, pl.ds(0, block_rows)], v_ref.at[dst], sems.at[slots + s]))
            for c in copies:
                c.start()
            for c in copies:
                c.wait()

        @pl.when(core_ref[0] == 0)
        def _():
            fetch(first_ref, second_ref)

        @pl.when(core_ref[0] != 0)
        def _():
            fetch(second_ref, first_ref)

        for b in range(k_ref.shape[0] // SPAN):
            vt_ref[b] = v_ref[b * SPAN:(b + 1) * SPAN, :].T

    own = own_ref[span]
    q_all = q_ref[...].reshape(nrow, heads * HD)
    for h in range(heads):
        qt_ref[:, h * nrow:(h + 1) * nrow] = q_all[:, h * HD:(h + 1) * HD].T

    def score(blk, g):
        keys = k_ref[pl.ds(pl.multiple_of(blk * SPAN, SPAN), SPAN), :]
        s = jnp.dot(keys, qt_ref[:, g * GW:(g + 1) * GW], preferred_element_type=jnp.float32)
        score_refs[g][...] = s
        top_ref[g] = jnp.max(s.reshape(SPAN // 8, 8, GW), axis=0)

    max_ref[...] = jnp.full_like(max_ref, MASKED)
    sum_ref[...] = jnp.zeros_like(sum_ref)
    acc_ref[...] = jnp.zeros_like(acc_ref)
    score(loc_ref[0], 0)

    def fold(s, top, blk, g):
        old = max_ref[g]
        new = jnp.maximum(old, jnp.broadcast_to(jnp.max(top, axis=0, keepdims=True), old.shape))
        max_ref[g] = new
        p = jnp.exp2(s.reshape(SPAN // 8, 8, GW) * LOG2_SCALE - (new * LOG2_SCALE)[None])
        factor = jnp.exp2((old - new) * LOG2_SCALE)
        sum_ref[g] = sum_ref[g] * factor + jnp.sum(p, axis=0)
        pv = jnp.dot(vt_ref[blk], p.reshape(SPAN, GW).astype(jnp.bfloat16), preferred_element_type=jnp.float32)
        acc_ref[g] = acc_ref[g] * factor[None] + pv.reshape(HD // 8, 8, GW)

    def body(t, carry):
        blk = loc_ref[t]
        for g in range(groups):
            if g + 1 < groups:
                score(blk, g + 1)
            else:
                score(loc_ref[t + 1], 0)
            fold(score_refs[g][...], top_ref[g], blk, g)
        return carry

    lax.fori_loop(0, own, body, 0)
    blk = loc_ref[own]
    key_i = lax.broadcasted_iota(jnp.int32, (SPAN, GW), 0)
    col_i = lax.broadcasted_iota(jnp.int32, (SPAN, GW), 1)
    for g in range(groups):
        if g + 1 < groups:
            score(blk, g + 1)
        r = (col_i + g * GW) & (nrow - 1)
        row_i = (r >> (rows.bit_length() - 1)) * run + part * rows + (r & (rows - 1))
        s = jnp.where(key_i <= row_i, score_refs[g][...], MASKED)
        fold(s, jnp.max(s.reshape(SPAN // 8, 8, GW), axis=0), blk, g)
    for g in range(groups):
        total = jnp.sum(sum_ref[g], axis=0, keepdims=True)
        done = (acc_ref[g].reshape(HD, GW) / total).T.astype(jnp.bfloat16)
        n = min(nrow, GW)
        for c in range(0, GW, n):
            h, r0 = divmod(g * GW + c, nrow)
            out_ref[r0 // rows:(r0 + n) // rows, :, h * HD:(h + 1) * HD] = done[c:c + n].reshape(n // rows, rows, HD)


def attend(own, loc, core, queries, first, second, part, tp_count):
    tok, width = queries.shape
    heads = width // HD
    run = tok // tp_count
    rows = run // PARTS
    spans = tok // SPAN
    per = tp_count // spans
    slots = first.shape[0]
    keys = slots * tok
    groups = per * rows * heads // GW
    pairs = heads * rows * per * spans * keys
    return pl.pallas_call(
        functools.partial(attend_kernel, rows=rows, part=part, heads=heads, run=run),
        out_shape=jax.ShapeDtypeStruct((tp_count, rows, width), jnp.bfloat16),
        grid_spec=pltpu.PrefetchScalarGridSpec(
            num_scalar_prefetch=3,
            grid=(spans,),
            in_specs=[
                pl.BlockSpec((per, rows, width), lambda s, *_: (s, part, 0)),
                pl.BlockSpec(memory_space=ANY),
                pl.BlockSpec(memory_space=ANY),
            ],
            out_specs=pl.BlockSpec((per, rows, width), lambda s, *_: (s, 0, 0)),
            scratch_shapes=[
                pltpu.VMEM((keys, HD), jnp.bfloat16),
                pltpu.VMEM((keys, HD), jnp.bfloat16),
                pltpu.VMEM((keys // SPAN, HD, SPAN), jnp.bfloat16),
                pltpu.VMEM((HD, per * rows * heads), jnp.bfloat16),
                pltpu.VMEM((groups, HD // 8, 8, GW), jnp.float32),
                pltpu.VMEM((groups, 8, GW), jnp.float32),
                pltpu.VMEM((groups, 8, GW), jnp.float32),
                pltpu.VMEM((groups, 8, GW), jnp.float32),
                pltpu.SemaphoreType.DMA((2 * slots,)),
            ]
            + [pltpu.VMEM((SPAN, GW), jnp.float32) for _ in range(groups)],
        ),
        compiler_params=pltpu.CompilerParams(dimension_semantics=("arbitrary",), vmem_limit_bytes=40 * 2**20),
        cost_estimate=pl.CostEstimate(flops=8 * HD * pairs, bytes_accessed=4 * keys * HD, transcendentals=pairs),
        name=f"attend{part}",
    )(own, loc, core, queries.reshape(tp_count, run, width), first, second)


def project_kernel(x_ref, *refs):
    att_refs, w_refs, out_refs = refs[:4], refs[4:8], refs[8:]
    step = pl.program_id(0)
    rows = out_refs[0].shape[0]
    total = None
    for a, w in zip(att_refs, w_refs):
        term = jnp.dot(a[...].reshape(rows, a.shape[-1]), w[...], preferred_element_type=jnp.float32)
        total = term if total is None else total + term
    for i, o in enumerate(out_refs):
        @pl.when(step == i)
        def _(o=o):
            o[...] = total.astype(jnp.bfloat16)


def project(x_rank, atts, ws):
    tps, r, k = atts[0].shape
    cores = tps // (2 * X_COUNT)
    n = ws[0].shape[1]
    rows = 2 * cores * r
    views = [a.reshape(2, X_COUNT, cores * r, k) for a in atts]
    pick = lambda i, x: (0, (x[0] + i) % X_COUNT, 0, 0)
    return pl.pallas_call(
        project_kernel,
        out_shape=[jax.ShapeDtypeStruct((rows, n), jnp.bfloat16)] * X_COUNT,
        grid_spec=pltpu.PrefetchScalarGridSpec(
            num_scalar_prefetch=1,
            grid=(X_COUNT,),
            in_specs=[pl.BlockSpec((2, 1, cores * r, k), pick)] * 4 + [pl.BlockSpec((k, n), lambda i, x: (0, 0))] * 4,
            out_specs=[pl.BlockSpec((rows, n), lambda i, x: (0, 0))] * X_COUNT,
        ),
        compiler_params=pltpu.CompilerParams(dimension_semantics=("arbitrary",), vmem_limit_bytes=56 * 2**20),
        cost_estimate=pl.CostEstimate(flops=2 * rows * X_COUNT * 4 * k * n, bytes_accessed=8 * k * n, transcendentals=0),
        name="project",
    )(x_rank, *views, *ws)


def gather_kernel(m_ref, *refs):
    ins, outs = refs[:4], refs[4:]
    step = pl.program_id(0)
    total = ins[0][...].astype(jnp.float32)
    for i in ins[1:]:
        total = total + i[...].astype(jnp.float32)
    for i, o in enumerate(outs):
        @pl.when(step == i)
        def _(o=o):
            o[...] = total.astype(jnp.bfloat16)


def add_parts(member, parts):
    rows, n = parts[0].shape
    r = rows // 4
    return pl.pallas_call(
        gather_kernel,
        out_shape=[jax.ShapeDtypeStruct((r, n), jnp.bfloat16)] * 4,
        grid_spec=pltpu.PrefetchScalarGridSpec(
            num_scalar_prefetch=1,
            grid=(4,),
            in_specs=[pl.BlockSpec((r, n), lambda i, m: (m[0] ^ i, 0))] * 4,
            out_specs=[pl.BlockSpec((r, n), lambda i, m: (0, 0))] * 4,
        ),
        compiler_params=pltpu.CompilerParams(dimension_semantics=("arbitrary",)),
        cost_estimate=pl.CostEstimate(flops=4 * rows * n, bytes_accessed=10 * rows * n, transcendentals=0),
        name="add_parts",
    )(member, *parts)


def finish_kernel(m_ref, scale_ref, res_ref, gain_ref, *refs):
    parts, hidden_ref, clipped_ref, tmp_ref = refs[:4], refs[4], refs[5], refs[6]
    n = parts[0].shape[1]
    square = None
    for i, part in enumerate(parts):
        cols = pl.ds(pl.multiple_of((m_ref[0] ^ i) * n, n), n)
        s = res_ref[:, cols].astype(jnp.float32) + part[...].astype(jnp.float32)
        tmp_ref[:, cols] = s
        hidden_ref[:, cols] = s.astype(jnp.bfloat16)
        t = jnp.sum(s * s, axis=1, keepdims=True)
        square = t if square is None else square + t
    inv = lax.rsqrt(square / (4 * n) + 1e-05)
    limit = 448.0 * scale_ref[0]
    clipped_ref[...] = jnp.clip(tmp_ref[...] * inv * gain_ref[...], -limit, limit).astype(jnp.bfloat16)


def finish(member, static_scale, residual, gain, parts):
    rows, width = residual.shape
    return pl.pallas_call(
        finish_kernel,
        out_shape=[jax.ShapeDtypeStruct((rows, width), jnp.bfloat16)] * 2,
        in_specs=[pl.BlockSpec(memory_space=pltpu.SMEM)] * 2 + [pl.BlockSpec(memory_space=pltpu.VMEM)] * 6,
        out_specs=[pl.BlockSpec(memory_space=pltpu.VMEM)] * 2,
        scratch_shapes=[pltpu.VMEM((rows, width), jnp.float32)],
        cost_estimate=pl.CostEstimate(flops=8 * rows * width, bytes_accessed=10 * rows * width, transcendentals=0),
        name="finish",
    )(member, static_scale, residual, gain, *parts)


def swapped(value, mask, count):
    return lax.ppermute(value, "tp", [(i, i ^ mask) for i in range(count)])


def shards(
    queries,
    context_keys,
    context_values,
    positions,
    out_weight,
    residual_in,
    norm_gain,
    static_scale,
):
    ctx_count = lax.axis_size("ctx")
    tp_count = lax.axis_size("tp")
    tp_rank = lax.axis_index("tp").astype(jnp.int32)
    tok, width = queries.shape
    core = tp_rank & 1
    x_rank = (tp_rank >> 1) & (X_COUNT - 1)
    far = tp_count // 2
    member = (tp_rank // far) * 2 + core
    masks = (0, 1, far, far + 1)

    kv_col = (tp_rank >> 1) * HD
    mine = jnp.where(
        core == 0,
        lax.dynamic_slice_in_dim(context_keys, kv_col, HD, 1),
        lax.dynamic_slice_in_dim(context_values, kv_col, HD, 1),
    )
    spans = tok // SPAN
    own = positions[::SPAN] // SPAN
    tag = jnp.pad(own.astype(jnp.bfloat16)[:, None] * jnp.ones((1, HD), jnp.bfloat16), ((0, 16 - spans), (0, 0)))
    mine = jnp.concatenate([mine, tag], axis=0)
    pieces = [mine]
    for dz in range(ctx_count // Y_COUNT):
        for dy in (0, 2, 1, 3):
            if dz or dy:
                pairs = [
                    (c, (c // Y_COUNT ^ dz) * Y_COUNT + (c + dy) % Y_COUNT) for c in range(ctx_count)
                ]
                pieces.append(lax.ppermute(mine, "ctx", pairs))
    first = jnp.stack(pieces)
    second = swapped(first, 1, tp_count)
    order = first[:, tok:tok + spans, 0].reshape(ctx_count * spans).astype(jnp.int32)
    blocks = jnp.arange(ctx_count * spans, dtype=jnp.int32)
    loc = jnp.sum(jnp.where(order[None, :] == blocks[:, None], blocks[None, :], 0), axis=1)

    quarter = out_weight.shape[1] // 4
    ws = []
    for i, mask in enumerate(masks):
        w = lax.dynamic_slice_in_dim(out_weight, (member ^ i) * quarter, quarter, 1)
        ws.append(swapped(w, mask, tp_count) if mask else w)

    outs = []
    for part in range(PARTS):
        att = attend(own, loc, core[None], queries, first, second, part, tp_count)
        atts = [swapped(att, mask, tp_count) if mask else att for mask in masks]
        sent = project(x_rank[None], atts, ws)
        got = [sent[0]]
        for dx in (2, 1, 3):
            pairs = []
            for t in range(tp_count):
                x = (t >> 1) & (X_COUNT - 1)
                pairs.append((t, t - 2 * x + 2 * ((x + dx) % X_COUNT)))
            got.append(lax.ppermute(sent[dx], "tp", pairs))
        cols = add_parts(member[None], got)
        cols = [swapped(c, mask, tp_count) if mask else c for c, mask in zip(cols, masks)]
        r = tok // tp_count // PARTS
        rows = slice(part * r, (part + 1) * r)
        outs.append(finish(member[None], static_scale, residual_in[rows], norm_gain[None, :], cols))
    return tuple(jnp.concatenate([o[i] for o in outs], axis=0) for i in range(2))


def solution(mesh):
    return jax.shard_map(
        shards,
        mesh=mesh,
        in_specs=(
            P("ctx", "tp"),
            P("ctx", None),
            P("ctx", None),
            P("ctx"),
            P("tp", None),
            P(("ctx", "tp"), None),
            P(),
            P(),
        ),
        out_specs=(P(("ctx", "tp"), None), P(("ctx", "tp"), None)),
        check_vma=False,
    )
```

```python
import functools
import math

import jax
import jax.numpy as jnp
from jax import lax
from jax.experimental import pallas as pl
from jax.experimental.pallas import tpu as pltpu
from jax.sharding import PartitionSpec as P


HD = 128
SPAN = 512
GW = 256
MASKED = -1e30
LOG2_SCALE = math.log2(math.e) / math.sqrt(HD)
PARTS = 2
Y_COUNT = 4
X_COUNT = 4
ANY = pl.ANY


def attend_kernel(
    own_ref, loc_ref, core_ref, q_ref, first_ref, second_ref, out_ref,
    k_ref, v_ref, vt_ref, qt_ref, acc_ref, max_ref, sum_ref, top_ref, factor_ref, sems, *tile_refs,
    rows, part, heads, run,
):
    span = pl.program_id(0)
    slots = first_ref.shape[0]
    block_rows = k_ref.shape[0] // slots
    nrow = q_ref.shape[0] * rows
    groups = nrow * heads // GW
    score_refs, weight_refs = tile_refs[:groups], tile_refs[groups:]

    @pl.when(span == 0)
    def _():
        def fetch(k_src, v_src):
            copies = []
            for s in range(slots):
                dst = pl.ds(s * block_rows, block_rows)
                copies.append(pltpu.make_async_copy(k_src.at[s, pl.ds(0, block_rows)], k_ref.at[dst], sems.at[s]))
                copies.append(pltpu.make_async_copy(v_src.at[s, pl.ds(0, block_rows)], v_ref.at[dst], sems.at[slots + s]))
            for c in copies:
                c.start()
            for c in copies:
                c.wait()

        @pl.when(core_ref[0] == 0)
        def _():
            fetch(first_ref, second_ref)

        @pl.when(core_ref[0] != 0)
        def _():
            fetch(second_ref, first_ref)

        for b in range(k_ref.shape[0] // SPAN):
            vt_ref[b] = v_ref[b * SPAN:(b + 1) * SPAN, :].T

    own = own_ref[span]
    q_all = q_ref[...].reshape(nrow, heads * HD)
    for h in range(heads):
        qt_ref[:, h * nrow:(h + 1) * nrow] = q_all[:, h * HD:(h + 1) * HD].T

    def score(blk, g):
        keys = k_ref[pl.ds(pl.multiple_of(blk * SPAN, SPAN), SPAN), :]
        s = jnp.dot(keys, qt_ref[:, g * GW:(g + 1) * GW], preferred_element_type=jnp.float32)
        score_refs[g][...] = s
        top_ref[g] = jnp.max(s.reshape(SPAN // 8, 8, GW), axis=0)

    def weigh(s, top, g):
        old = max_ref[g]
        new = jnp.maximum(old, jnp.broadcast_to(jnp.max(top, axis=0, keepdims=True), old.shape))
        max_ref[g] = new
        p = jnp.exp2(s.reshape(SPAN // 8, 8, GW) * LOG2_SCALE - (new * LOG2_SCALE)[None])
        factor = jnp.exp2((old - new) * LOG2_SCALE)
        factor_ref[g] = factor
        sum_ref[g] = sum_ref[g] * factor + jnp.sum(p, axis=0)
        weight_refs[g][...] = p.reshape(SPAN, GW).astype(jnp.bfloat16)

    def apply(blk, g):
        pv = jnp.dot(vt_ref[blk], weight_refs[g][...], preferred_element_type=jnp.float32)
        acc_ref[g] = acc_ref[g] * factor_ref[g][None] + pv.reshape(HD // 8, 8, GW)

    max_ref[...] = jnp.full_like(max_ref, MASKED)
    sum_ref[...] = jnp.zeros_like(sum_ref)
    acc_ref[...] = jnp.zeros_like(acc_ref)
    factor_ref[...] = jnp.zeros_like(factor_ref)
    for g in range(groups):
        weight_refs[g][...] = jnp.zeros_like(weight_refs[g])
        score(loc_ref[0], g)

    def body(t, carry):
        prev = loc_ref[jnp.maximum(t - 1, 0)]
        for g in range(groups):
            apply(prev, g)
            weigh(score_refs[g][...], top_ref[g], g)
            score(loc_ref[t + 1], g)
        return carry

    lax.fori_loop(0, own, body, 0)
    prev = loc_ref[jnp.maximum(own - 1, 0)]
    key_i = lax.broadcasted_iota(jnp.int32, (SPAN, GW), 0)
    col_i = lax.broadcasted_iota(jnp.int32, (SPAN, GW), 1)
    for g in range(groups):
        apply(prev, g)
        r = (col_i + g * GW) & (nrow - 1)
        row_i = (r >> (rows.bit_length() - 1)) * run + part * rows + (r & (rows - 1))
        s = jnp.where(key_i <= row_i, score_refs[g][...], MASKED)
        weigh(s, jnp.max(s.reshape(SPAN // 8, 8, GW), axis=0), g)
    for g in range(groups):
        apply(loc_ref[own], g)
    for g in range(groups):
        total = jnp.sum(sum_ref[g], axis=0, keepdims=True)
        done = (acc_ref[g].reshape(HD, GW) * (1.0 / total)).T.astype(jnp.bfloat16)
        n = min(nrow, GW)
        for c in range(0, GW, n):
            h, r0 = divmod(g * GW + c, nrow)
            out_ref[r0 // rows:(r0 + n) // rows, :, h * HD:(h + 1) * HD] = done[c:c + n].reshape(n // rows, rows, HD)


def attend(own, loc, core, queries, first, second, part, tp_count):
    tok, width = queries.shape
    heads = width // HD
    run = tok // tp_count
    rows = run // PARTS
    spans = tok // SPAN
    per = tp_count // spans
    slots = first.shape[0]
    keys = slots * tok
    groups = per * rows * heads // GW
    pairs = heads * rows * per * spans * keys
    return pl.pallas_call(
        functools.partial(attend_kernel, rows=rows, part=part, heads=heads, run=run),
        out_shape=jax.ShapeDtypeStruct((tp_count, rows, width), jnp.bfloat16),
        grid_spec=pltpu.PrefetchScalarGridSpec(
            num_scalar_prefetch=3,
            grid=(spans,),
            in_specs=[
                pl.BlockSpec((per, rows, width), lambda s, *_: (s, part, 0)),
                pl.BlockSpec(memory_space=ANY),
                pl.BlockSpec(memory_space=ANY),
            ],
            out_specs=pl.BlockSpec((per, rows, width), lambda s, *_: (s, 0, 0)),
            scratch_shapes=[
                pltpu.VMEM((keys, HD), jnp.bfloat16),
                pltpu.VMEM((keys, HD), jnp.bfloat16),
                pltpu.VMEM((keys // SPAN, HD, SPAN), jnp.bfloat16),
                pltpu.VMEM((HD, per * rows * heads), jnp.bfloat16),
                pltpu.VMEM((groups, HD // 8, 8, GW), jnp.float32),
                pltpu.VMEM((groups, 8, GW), jnp.float32),
                pltpu.VMEM((groups, 8, GW), jnp.float32),
                pltpu.VMEM((groups, 8, GW), jnp.float32),
                pltpu.VMEM((groups, 8, GW), jnp.float32),
                pltpu.SemaphoreType.DMA((2 * slots,)),
            ]
            + [pltpu.VMEM((SPAN, GW), jnp.float32)] * groups
            + [pltpu.VMEM((SPAN, GW), jnp.bfloat16)] * groups,
        ),
        compiler_params=pltpu.CompilerParams(dimension_semantics=("arbitrary",), vmem_limit_bytes=40 * 2**20),
        cost_estimate=pl.CostEstimate(flops=8 * HD * pairs, bytes_accessed=4 * keys * HD, transcendentals=pairs),
    )(own, loc, core, queries.reshape(tp_count, run, width), first, second)


def project_kernel(x_ref, *refs):
    att_refs, w_refs, out_refs = refs[:4], refs[4:8], refs[8:]
    step = pl.program_id(0)
    rows = out_refs[0].shape[0]
    total = None
    for a, w in zip(att_refs, w_refs):
        term = jnp.dot(a[...].reshape(rows, a.shape[-1]), w[...], preferred_element_type=jnp.float32)
        total = term if total is None else total + term
    for i, o in enumerate(out_refs):
        @pl.when(step == i)
        def _(o=o):
            o[...] = total.astype(jnp.bfloat16)


def project(x_rank, atts, ws):
    tps, r, k = atts[0].shape
    cores = tps // (2 * X_COUNT)
    n = ws[0].shape[1]
    rows = 2 * cores * r
    views = [a.reshape(2, X_COUNT, cores * r, k) for a in atts]
    pick = lambda i, x: (0, (x[0] + i) % X_COUNT, 0, 0)
    return pl.pallas_call(
        project_kernel,
        out_shape=[jax.ShapeDtypeStruct((rows, n), jnp.bfloat16)] * X_COUNT,
        grid_spec=pltpu.PrefetchScalarGridSpec(
            num_scalar_prefetch=1,
            grid=(X_COUNT,),
            in_specs=[pl.BlockSpec((2, 1, cores * r, k), pick)] * 4 + [pl.BlockSpec((k, n), lambda i, x: (0, 0))] * 4,
            out_specs=[pl.BlockSpec((rows, n), lambda i, x: (0, 0))] * X_COUNT,
        ),
        compiler_params=pltpu.CompilerParams(dimension_semantics=("arbitrary",), vmem_limit_bytes=56 * 2**20),
        cost_estimate=pl.CostEstimate(flops=2 * rows * X_COUNT * 4 * k * n, bytes_accessed=8 * k * n, transcendentals=0),
        name="project",
    )(x_rank, *views, *ws)


def gather_kernel(m_ref, *refs):
    ins, outs = refs[:4], refs[4:]
    step = pl.program_id(0)
    total = ins[0][...].astype(jnp.float32)
    for i in ins[1:]:
        total = total + i[...].astype(jnp.float32)
    for i, o in enumerate(outs):
        @pl.when(step == i)
        def _(o=o):
            o[...] = total.astype(jnp.bfloat16)


def add_parts(member, parts):
    rows, n = parts[0].shape
    r = rows // 4
    return pl.pallas_call(
        gather_kernel,
        out_shape=[jax.ShapeDtypeStruct((r, n), jnp.bfloat16)] * 4,
        grid_spec=pltpu.PrefetchScalarGridSpec(
            num_scalar_prefetch=1,
            grid=(4,),
            in_specs=[pl.BlockSpec((r, n), lambda i, m: (m[0] ^ i, 0))] * 4,
            out_specs=[pl.BlockSpec((r, n), lambda i, m: (0, 0))] * 4,
        ),
        compiler_params=pltpu.CompilerParams(dimension_semantics=("arbitrary",)),
        cost_estimate=pl.CostEstimate(flops=4 * rows * n, bytes_accessed=10 * rows * n, transcendentals=0),
        name="add_parts",
    )(member, *parts)


def finish_kernel(m_ref, scale_ref, res_ref, gain_ref, *refs):
    parts, (hidden_ref, clipped_ref, tmp_ref) = refs[:4], refs[4:]
    n = parts[0].shape[1]
    square = None
    for i, part in enumerate(parts):
        cols = pl.ds(pl.multiple_of((m_ref[0] ^ i) * n, n), n)
        s = res_ref[:, cols].astype(jnp.float32) + part[...].astype(jnp.float32)
        tmp_ref[:, cols] = s
        hidden_ref[:, cols] = s.astype(jnp.bfloat16)
        t = jnp.sum(s * s, axis=1, keepdims=True)
        square = t if square is None else square + t
    inv = lax.rsqrt(square / (4 * n) + 1e-05)
    limit = 448.0 * scale_ref[0]
    clipped_ref[...] = jnp.clip(tmp_ref[...] * inv * gain_ref[...], -limit, limit).astype(jnp.bfloat16)


def finish(member, static_scale, residual, gain, parts, part, before):
    rows, width = residual.shape
    r = rows // PARTS
    whole = pl.BlockSpec((r, width), lambda i, *_: (part, 0))
    small = pl.BlockSpec(parts[0].shape, lambda i, *_: (0, 0))
    kernel = finish_kernel
    if before:
        kernel = lambda m, s, res, g, a, b, c, d, e, f, *rest: finish_kernel(m, s, res, g, a, b, c, d, *rest)
    return pl.pallas_call(
        kernel,
        out_shape=[jax.ShapeDtypeStruct((rows, width), jnp.bfloat16)] * 2,
        grid_spec=pltpu.PrefetchScalarGridSpec(
            num_scalar_prefetch=2,
            grid=(1,),
            in_specs=[whole, pl.BlockSpec((1, width), lambda i, *_: (0, 0))]
            + [small] * 4
            + [pl.BlockSpec(memory_space=ANY)] * len(before),
            out_specs=[whole] * 2,
            scratch_shapes=[pltpu.VMEM((r, width), jnp.float32)],
        ),
        input_output_aliases={8 + i: i for i in range(len(before))},
        cost_estimate=pl.CostEstimate(flops=8 * r * width, bytes_accessed=10 * r * width, transcendentals=0),
    )(member, static_scale, residual, gain, *parts, *before)


def swapped(value, mask, count):
    return lax.ppermute(value, "tp", [(i, i ^ mask) for i in range(count)])


def shards(
    queries,
    context_keys,
    context_values,
    positions,
    out_weight,
    residual_in,
    norm_gain,
    static_scale,
):
    ctx_count = lax.axis_size("ctx")
    tp_count = lax.axis_size("tp")
    tp_rank = lax.axis_index("tp").astype(jnp.int32)
    tok, _ = queries.shape
    core = tp_rank & 1
    x_rank = (tp_rank >> 1) & (X_COUNT - 1)
    far = tp_count // 2
    member = (tp_rank // far) * 2 + core
    masks = (0, 1, far, far + 1)

    kv_col = (tp_rank >> 1) * HD
    mine = jnp.where(
        core == 0,
        lax.dynamic_slice_in_dim(context_keys, kv_col, HD, 1),
        lax.dynamic_slice_in_dim(context_values, kv_col, HD, 1),
    )
    spans = tok // SPAN
    own = positions[::SPAN] // SPAN
    tag = jnp.pad(own.astype(jnp.bfloat16)[:, None] * jnp.ones((1, HD), jnp.bfloat16), ((0, 16 - spans), (0, 0)))
    mine = jnp.concatenate([mine, tag], axis=0)
    pieces = [mine]
    for dz in range(ctx_count // Y_COUNT):
        for dy in (0, 2, 1, 3):
            if dz or dy:
                pairs = [
                    (c, (c // Y_COUNT ^ dz) * Y_COUNT + (c + dy) % Y_COUNT) for c in range(ctx_count)
                ]
                pieces.append(lax.ppermute(mine, "ctx", pairs))
    first = jnp.stack(pieces)
    second = swapped(first, 1, tp_count)
    order = first[:, tok:tok + spans, 0].reshape(ctx_count * spans).astype(jnp.int32)
    blocks = jnp.arange(ctx_count * spans, dtype=jnp.int32)
    loc = jnp.sum(jnp.where(order[None, :] == blocks[:, None], blocks[None, :], 0), axis=1)

    quarter = out_weight.shape[1] // 4
    ws = []
    for i, mask in enumerate(masks):
        w = lax.dynamic_slice_in_dim(out_weight, (member ^ i) * quarter, quarter, 1)
        ws.append(swapped(w, mask, tp_count) if mask else w)

    outs = ()
    for part in range(PARTS):
        att = attend(own, loc, core[None], queries, first, second, part, tp_count)
        atts = []
        for mask in masks:
            atts.append(swapped(att, mask, tp_count) if mask else att)
        sent = project(x_rank[None], atts, ws)
        got = [sent[0]]
        for dx in (2, 1, 3):
            pairs = []
            for t in range(tp_count):
                x = (t >> 1) & (X_COUNT - 1)
                pairs.append((t, t - 2 * x + 2 * ((x + dx) % X_COUNT)))
            got.append(lax.ppermute(sent[dx], "tp", pairs))
        cols = list(add_parts(member[None], got))
        for i, mask in enumerate(masks):
            if mask:
                cols[i] = swapped(cols[i], mask, tp_count)
        outs = finish(member[None], static_scale, residual_in, norm_gain[None, :], cols, part, outs)
    return tuple(outs)


def solution(mesh):
    return jax.shard_map(
        shards,
        mesh=mesh,
        in_specs=(
            P("ctx", "tp"),
            P("ctx", None),
            P("ctx", None),
            P("ctx"),
            P("tp", None),
            P(("ctx", "tp"), None),
            P(),
            P(),
        ),
        out_specs=(P(("ctx", "tp"), None), P(("ctx", "tp"), None)),
        check_vma=False,
    )
```

```python
import functools
import math

import jax
import jax.numpy as jnp
from jax import lax
from jax.experimental import pallas as pl
from jax.experimental.pallas import tpu as pltpu
from jax.sharding import PartitionSpec as P


HD = 128
SPAN = 512
GW = 256
MASKED = -1e30
LOG2_SCALE = math.log2(math.e) / math.sqrt(HD)
PARTS = 2
Y_COUNT = 4
ANY = pl.ANY


def attend_kernel(
    own_ref, loc_ref, core_ref, q_ref, first_ref, second_ref, out_ref,
    k_ref, v_ref, vt_ref, qt_ref, acc_ref, max_ref, sum_ref, top_ref, factor_ref, sems, *tile_refs,
    rows, part, heads, run,
):
    span = pl.program_id(0)
    slots = first_ref.shape[0]
    block_rows = k_ref.shape[0] // slots
    nrow = q_ref.shape[0] * rows
    groups = nrow * heads // GW
    score_refs, weight_refs = tile_refs[:groups], tile_refs[groups:]

    @pl.when(span == 0)
    def _():
        def fetch(k_src, v_src):
            copies = []
            for s in range(slots):
                dst = pl.ds(s * block_rows, block_rows)
                copies.append(pltpu.make_async_copy(k_src.at[s, pl.ds(0, block_rows)], k_ref.at[dst], sems.at[s]))
                copies.append(pltpu.make_async_copy(v_src.at[s, pl.ds(0, block_rows)], v_ref.at[dst], sems.at[slots + s]))
            for c in copies:
                c.start()
            for c in copies:
                c.wait()

        @pl.when(core_ref[0] == 0)
        def _():
            fetch(first_ref, second_ref)

        @pl.when(core_ref[0] != 0)
        def _():
            fetch(second_ref, first_ref)

        for b in range(k_ref.shape[0] // SPAN):
            vt_ref[b] = v_ref[b * SPAN:(b + 1) * SPAN, :].T

    own = own_ref[span]
    q_all = q_ref[...].reshape(nrow, heads * HD)
    for h in range(heads):
        qt_ref[:, h * nrow:(h + 1) * nrow] = q_all[:, h * HD:(h + 1) * HD].T

    def score(blk, g):
        keys = k_ref[pl.ds(pl.multiple_of(blk * SPAN, SPAN), SPAN), :]
        s = jnp.dot(keys, qt_ref[:, g * GW:(g + 1) * GW], preferred_element_type=jnp.float32)
        score_refs[g][...] = s
        top_ref[g] = jnp.max(s.reshape(SPAN // 8, 8, GW), axis=0)

    def weigh(s, top, g):
        old = max_ref[g]
        new = jnp.maximum(old, jnp.broadcast_to(jnp.max(top, axis=0, keepdims=True), old.shape))
        max_ref[g] = new
        p = jnp.exp2(s.reshape(SPAN // 8, 8, GW) * LOG2_SCALE - (new * LOG2_SCALE)[None])
        factor = jnp.exp2((old - new) * LOG2_SCALE)
        factor_ref[g] = factor
        sum_ref[g] = sum_ref[g] * factor + jnp.sum(p, axis=0)
        weight_refs[g][...] = p.reshape(SPAN, GW).astype(jnp.bfloat16)

    def apply(blk, g):
        pv = jnp.dot(vt_ref[blk], weight_refs[g][...], preferred_element_type=jnp.float32)
        acc_ref[g] = acc_ref[g] * factor_ref[g][None] + pv.reshape(HD // 8, 8, GW)

    max_ref[...] = jnp.full_like(max_ref, MASKED)
    sum_ref[...] = jnp.zeros_like(sum_ref)
    acc_ref[...] = jnp.zeros_like(acc_ref)
    factor_ref[...] = jnp.zeros_like(factor_ref)
    for g in range(groups):
        weight_refs[g][...] = jnp.zeros_like(weight_refs[g])
        score(loc_ref[0], g)

    def body(t, carry):
        prev = loc_ref[jnp.maximum(t - 1, 0)]
        for g in range(groups):
            apply(prev, g)
            weigh(score_refs[g][...], top_ref[g], g)
            score(loc_ref[t + 1], g)
        return carry

    lax.fori_loop(0, own, body, 0)
    prev = loc_ref[jnp.maximum(own - 1, 0)]
    key_i = lax.broadcasted_iota(jnp.int32, (SPAN, GW), 0)
    col_i = lax.broadcasted_iota(jnp.int32, (SPAN, GW), 1)
    for g in range(groups):
        apply(prev, g)
        r = (col_i + g * GW) & (nrow - 1)
        row_i = (r >> (rows.bit_length() - 1)) * run + part * rows + (r & (rows - 1))
        s = jnp.where(key_i <= row_i, score_refs[g][...], MASKED)
        weigh(s, jnp.max(s.reshape(SPAN // 8, 8, GW), axis=0), g)
    for g in range(groups):
        apply(loc_ref[own], g)
    for g in range(groups):
        total = jnp.sum(sum_ref[g], axis=0, keepdims=True)
        done = (acc_ref[g].reshape(HD, GW) * (1.0 / total)).T.astype(jnp.bfloat16)
        n = min(nrow, GW)
        for c in range(0, GW, n):
            h, r0 = divmod(g * GW + c, nrow)
            out_ref[r0 // rows:(r0 + n) // rows, :, h * HD:(h + 1) * HD] = done[c:c + n].reshape(n // rows, rows, HD)


def attend(own, loc, core, queries, first, second, part, tp_count):
    tok, width = queries.shape
    heads = width // HD
    run = tok // tp_count
    rows = run // PARTS
    spans = tok // SPAN
    per = tp_count // spans
    slots = first.shape[0]
    keys = slots * tok
    groups = per * rows * heads // GW
    pairs = heads * rows * per * spans * keys
    return pl.pallas_call(
        functools.partial(attend_kernel, rows=rows, part=part, heads=heads, run=run),
        out_shape=jax.ShapeDtypeStruct((tp_count, rows, width), jnp.bfloat16),
        grid_spec=pltpu.PrefetchScalarGridSpec(
            num_scalar_prefetch=3,
            grid=(spans,),
            in_specs=[
                pl.BlockSpec((per, rows, width), lambda s, *_: (s, part, 0)),
                pl.BlockSpec(memory_space=ANY),
                pl.BlockSpec(memory_space=ANY),
            ],
            out_specs=pl.BlockSpec((per, rows, width), lambda s, *_: (s, 0, 0)),
            scratch_shapes=[
                pltpu.VMEM((keys, HD), jnp.bfloat16),
                pltpu.VMEM((keys, HD), jnp.bfloat16),
                pltpu.VMEM((keys // SPAN, HD, SPAN), jnp.bfloat16),
                pltpu.VMEM((HD, per * rows * heads), jnp.bfloat16),
                pltpu.VMEM((groups, HD // 8, 8, GW), jnp.float32),
                pltpu.VMEM((groups, 8, GW), jnp.float32),
                pltpu.VMEM((groups, 8, GW), jnp.float32),
                pltpu.VMEM((groups, 8, GW), jnp.float32),
                pltpu.VMEM((groups, 8, GW), jnp.float32),
                pltpu.SemaphoreType.DMA((2 * slots,)),
            ]
            + [pltpu.VMEM((SPAN, GW), jnp.float32)] * groups
            + [pltpu.VMEM((SPAN, GW), jnp.bfloat16)] * groups,
        ),
        compiler_params=pltpu.CompilerParams(dimension_semantics=("arbitrary",), vmem_limit_bytes=40 * 2**20),
        cost_estimate=pl.CostEstimate(flops=8 * HD * pairs, bytes_accessed=4 * keys * HD, transcendentals=pairs),
    )(own, loc, core, queries.reshape(tp_count, run, width), first, second)


def stack_kernel(*refs):
    ins, out_ref, sems = refs[:-2], refs[-2], refs[-1]
    copies = [pltpu.make_async_copy(x, out_ref.at[i], sems.at[i]) for i, x in enumerate(ins)]
    for c in copies:
        c.start()
    for c in copies:
        c.wait()


def stacked(pieces):
    shape = (len(pieces), *pieces[0].shape)
    return pl.pallas_call(
        stack_kernel,
        out_shape=jax.ShapeDtypeStruct(shape, pieces[0].dtype),
        in_specs=[pl.BlockSpec(memory_space=ANY)] * len(pieces),
        out_specs=pl.BlockSpec(memory_space=ANY),
        scratch_shapes=[pltpu.SemaphoreType.DMA((len(pieces),))],
    )(*pieces)


def project_kernel(place_ref, *refs):
    atts, near, far, (acc_ref,), outs = refs[:4], refs[4:6], refs[6:10], refs[14:], refs[10:14]
    step = pl.program_id(0)
    rows, k = acc_ref.shape[0], atts[0].shape[-1]
    near_term = jnp.dot(atts[0][...].reshape(rows, k), near[0][...], preferred_element_type=jnp.float32)
    near_term += jnp.dot(atts[1][...].reshape(rows, k), near[1][...], preferred_element_type=jnp.float32)
    for j, w in enumerate(far):
        @pl.when(step == j)
        def _(w=w):
            total = near_term + jnp.dot(atts[2][...].reshape(rows, k), w[0], preferred_element_type=jnp.float32)
            acc_ref[...] = total + jnp.dot(atts[3][...].reshape(rows, k), w[1], preferred_element_type=jnp.float32)
    n = outs[0].shape[0]
    for i, o in enumerate(outs):
        o[...] = acc_ref[pl.ds(pl.multiple_of((place_ref[1] ^ i) * n, n), n), :].astype(jnp.bfloat16)


def project(place, atts, weight, paired, far):
    tps, r, k = atts[0].shape
    rows, cut = tps * r, far[0].shape[-1]
    blocks = len(far)
    col = lambda j, p: (p[2] - j) & (blocks - 1)
    return pl.pallas_call(
        project_kernel,
        out_shape=[jax.ShapeDtypeStruct((rows // 4, cut * blocks), jnp.bfloat16)] * 4,
        grid_spec=pltpu.PrefetchScalarGridSpec(
            num_scalar_prefetch=1,
            grid=(blocks,),
            in_specs=[pl.BlockSpec((tps, r, k), lambda j, p: (0, 0, 0))] * 4
            + [
                pl.BlockSpec((k, cut), lambda j, p: (0, p[0] * blocks + col(j, p))),
                pl.BlockSpec((k, cut), lambda j, p: (0, col(j, p))),
            ]
            + [pl.BlockSpec(far[0].shape, lambda j, p: (0, 0, 0))] * blocks,
            out_specs=[pl.BlockSpec((rows // 4, cut), lambda j, p: (0, col(j, p)))] * 4,
            scratch_shapes=[pltpu.VMEM((rows, cut), jnp.float32)],
        ),
        compiler_params=pltpu.CompilerParams(dimension_semantics=("arbitrary",), vmem_limit_bytes=40 * 2**20),
        cost_estimate=pl.CostEstimate(flops=8 * rows * k * cut * blocks, bytes_accessed=8 * k * cut * blocks, transcendentals=0),
        name="project",
    )(place, *atts, weight, paired, *far)


def gather_kernel(m_ref, *refs):
    ins, outs = refs[:4], refs[4:]
    step = pl.program_id(0)
    total = ins[0][...].astype(jnp.float32)
    for i in ins[1:]:
        total = total + i[...].astype(jnp.float32)
    for i, o in enumerate(outs):
        @pl.when(step == i)
        def _(o=o):
            o[...] = total.astype(jnp.bfloat16)


def add_parts(member, parts):
    rows, n = parts[0].shape
    r = rows // 4
    return pl.pallas_call(
        gather_kernel,
        out_shape=[jax.ShapeDtypeStruct((r, n), jnp.bfloat16)] * 4,
        grid_spec=pltpu.PrefetchScalarGridSpec(
            num_scalar_prefetch=1,
            grid=(4,),
            in_specs=[pl.BlockSpec((r, n), lambda i, m: (m[0] ^ i, 0))] * 4,
            out_specs=[pl.BlockSpec((r, n), lambda i, m: (0, 0))] * 4,
        ),
        compiler_params=pltpu.CompilerParams(dimension_semantics=("arbitrary",)),
        cost_estimate=pl.CostEstimate(flops=4 * rows * n, bytes_accessed=10 * rows * n, transcendentals=0),
        name="add_parts",
    )(member, *parts)


def finish_kernel(m_ref, scale_ref, res_ref, gain_ref, *refs):
    parts, (hidden_ref, clipped_ref, tmp_ref) = refs[:4], refs[4:]
    n = parts[0].shape[1]
    square = None
    for i, part in enumerate(parts):
        cols = pl.ds(pl.multiple_of((m_ref[0] ^ i) * n, n), n)
        s = res_ref[:, cols].astype(jnp.float32) + part[...].astype(jnp.float32)
        tmp_ref[:, cols] = s
        hidden_ref[:, cols] = s.astype(jnp.bfloat16)
        t = jnp.sum(s * s, axis=1, keepdims=True)
        square = t if square is None else square + t
    inv = lax.rsqrt(square / (4 * n) + 1e-05)
    limit = 448.0 * scale_ref[0]
    clipped_ref[...] = jnp.clip(tmp_ref[...] * inv * gain_ref[...], -limit, limit).astype(jnp.bfloat16)


def finish(member, static_scale, residual, gain, parts, part, before):
    rows, width = residual.shape
    r = rows // PARTS
    whole = pl.BlockSpec((r, width), lambda i, *_: (part, 0))
    small = pl.BlockSpec(parts[0].shape, lambda i, *_: (0, 0))
    kernel = finish_kernel
    if before:
        kernel = lambda m, s, res, g, a, b, c, d, e, f, *rest: finish_kernel(m, s, res, g, a, b, c, d, *rest)
    return pl.pallas_call(
        kernel,
        out_shape=[jax.ShapeDtypeStruct((rows, width), jnp.bfloat16)] * 2,
        grid_spec=pltpu.PrefetchScalarGridSpec(
            num_scalar_prefetch=2,
            grid=(1,),
            in_specs=[whole, pl.BlockSpec((1, width), lambda i, *_: (0, 0))]
            + [small] * 4
            + [pl.BlockSpec(memory_space=ANY)] * len(before),
            out_specs=[whole] * 2,
            scratch_shapes=[pltpu.VMEM((r, width), jnp.float32)],
        ),
        input_output_aliases={8 + i: i for i in range(len(before))},
        cost_estimate=pl.CostEstimate(flops=8 * r * width, bytes_accessed=10 * r * width, transcendentals=0),
    )(member, static_scale, residual, gain, *parts, *before)


def swapped(value, mask, count):
    return lax.ppermute(value, "tp", [(i, i ^ mask) for i in range(count)])


def shards(
    queries,
    context_keys,
    context_values,
    positions,
    out_weight,
    residual_in,
    norm_gain,
    static_scale,
):
    ctx_count = lax.axis_size("ctx")
    tp_count = lax.axis_size("tp")
    tp_rank = lax.axis_index("tp").astype(jnp.int32)
    tok, _ = queries.shape
    core = tp_rank & 1
    member = tp_rank & 3
    group = tp_rank >> 2
    y_rank = lax.axis_index("ctx").astype(jnp.int32) & (Y_COUNT - 1)

    kv_col = (tp_rank >> 1) * HD
    mine = jnp.where(
        core == 0,
        lax.dynamic_slice_in_dim(context_keys, kv_col, HD, 1),
        lax.dynamic_slice_in_dim(context_values, kv_col, HD, 1),
    )
    spans = tok // SPAN
    own = positions[::SPAN] // SPAN
    tag = jnp.pad(own.astype(jnp.bfloat16)[:, None] * jnp.ones((1, HD), jnp.bfloat16), ((0, 16 - spans), (0, 0)))
    mine = jnp.concatenate([mine, tag], axis=0)
    pieces = [mine]
    for dz in range(ctx_count // Y_COUNT):
        for dy in (0, 2, 1, 3):
            if dz or dy:
                pairs = [
                    (c, (c // Y_COUNT ^ dz) * Y_COUNT + (c + dy) % Y_COUNT) for c in range(ctx_count)
                ]
                pieces.append(lax.ppermute(mine, "ctx", pairs))
    first = stacked(pieces)
    second = swapped(first, 1, tp_count)
    order = first[:, tok:tok + spans, 0].reshape(ctx_count * spans).astype(jnp.int32)
    blocks = jnp.arange(ctx_count * spans, dtype=jnp.int32)
    loc = jnp.sum(jnp.where(order[None, :] == blocks[:, None], blocks[None, :], 0), axis=1)

    quarter = out_weight.shape[1] // 4
    cut = quarter // Y_COUNT
    sides = []
    for i in (2, 3):
        w = lax.dynamic_slice_in_dim(out_weight, (member ^ i) * quarter + y_rank * cut, cut, 1)
        sides.append(swapped(w, i, tp_count))
    side = stacked(sides)
    far = [side]
    for dy in (1, 2, 3):
        pairs = [(c, c - c % Y_COUNT + (c + dy) % Y_COUNT) for c in range(ctx_count)]
        far.append(lax.ppermute(side, "ctx", pairs))
    w = lax.dynamic_slice_in_dim(out_weight, (member ^ 1) * quarter, quarter, 1)
    paired = swapped(w, 1, tp_count)
    place = jnp.stack([member, group, y_rank])

    outs = ()
    for part in range(PARTS):
        att = attend(own, loc, core[None], queries, first, second, part, tp_count)
        atts = [att]
        for i in (1, 2, 3):
            atts.append(swapped(att, i, tp_count))
        sent = project(place, atts, out_weight, paired, far)
        got = [sent[0]]
        for i in (1, 2, 3):
            got.append(swapped(sent[i], 4 * i, tp_count))
        cols = list(add_parts(member[None], got))
        for i in (1, 2, 3):
            cols[i] = swapped(cols[i], i, tp_count)
        outs = finish(member[None], static_scale, residual_in, norm_gain[None, :], cols, part, outs)
    return tuple(outs)


def solution(mesh):
    return jax.shard_map(
        shards,
        mesh=mesh,
        in_specs=(
            P("ctx", "tp"),
            P("ctx", None),
            P("ctx", None),
            P("ctx"),
            P("tp", None),
            P(("ctx", "tp"), None),
            P(),
            P(),
        ),
        out_specs=(P(("ctx", "tp"), None), P(("ctx", "tp"), None)),
        check_vma=False,
    )
```

```python
import functools
import math

import jax
import jax.numpy as jnp
from jax import lax
from jax.experimental import pallas as pl
from jax.experimental.pallas import tpu as pltpu
from jax.sharding import PartitionSpec as P


HD = 128
SPAN = 512
GW = 256
MASKED = -1e30
LOG2_SCALE = math.log2(math.e) / math.sqrt(HD)
PARTS = 2
Y_COUNT = 4
ANY = pl.ANY
VMEM_SPEC = pl.BlockSpec(memory_space=pltpu.VMEM)


def attend_kernel(
    own_ref, loc_ref, core_ref, q_ref, first_ref, second_ref, out_ref,
    k_ref, vt_ref, qt_ref, acc_ref, max_ref, sum_ref, top_ref, factor_ref, *tile_refs,
    rows, part, heads, run,
):
    span = pl.program_id(0)
    slots = first_ref.shape[0]
    block_rows = k_ref.shape[0] // slots
    nrow = q_ref.shape[0] * rows
    groups = nrow * heads // GW
    score_refs, weight_refs = tile_refs[:groups], tile_refs[groups:]

    @pl.when(span == 0)
    def _():
        def take(keys, values):
            for i in range(slots):
                at = i * block_rows
                k_ref[at:at + block_rows, :] = keys[i, :block_rows, :]
                for b in range(0, block_rows, SPAN):
                    vt_ref[(at + b) // SPAN] = values[i, b:b + SPAN, :].T

        @pl.when(core_ref[0] == 0)
        def _():
            take(first_ref, second_ref)

        @pl.when(core_ref[0] != 0)
        def _():
            take(second_ref, first_ref)

    own = own_ref[span]
    q_all = q_ref[...].reshape(nrow, heads * HD)
    for h in range(heads):
        qt_ref[:, h * nrow:(h + 1) * nrow] = q_all[:, h * HD:(h + 1) * HD].T

    def score(blk, g):
        keys = k_ref[pl.ds(pl.multiple_of(blk * SPAN, SPAN), SPAN), :]
        s = jnp.dot(keys, qt_ref[:, g * GW:(g + 1) * GW], preferred_element_type=jnp.float32)
        score_refs[g][...] = s
        top_ref[g] = jnp.max(s.reshape(SPAN // 8, 8, GW), axis=0)

    def weigh(s, top, g):
        old = max_ref[g]
        new = jnp.maximum(old, jnp.broadcast_to(jnp.max(top, axis=0, keepdims=True), old.shape))
        max_ref[g] = new
        p = jnp.exp2(s.reshape(SPAN // 8, 8, GW) * LOG2_SCALE - (new * LOG2_SCALE)[None])
        factor = jnp.exp2((old - new) * LOG2_SCALE)
        factor_ref[g] = factor
        sum_ref[g] = sum_ref[g] * factor + jnp.sum(p, axis=0)
        weight_refs[g][...] = p.reshape(SPAN, GW).astype(jnp.bfloat16)

    def apply(blk, g):
        pv = jnp.dot(vt_ref[blk], weight_refs[g][...], preferred_element_type=jnp.float32)
        acc_ref[g] = acc_ref[g] * factor_ref[g][None] + pv.reshape(HD // 8, 8, GW)

    max_ref[...] = jnp.full_like(max_ref, MASKED)
    sum_ref[...] = jnp.zeros_like(sum_ref)
    acc_ref[...] = jnp.zeros_like(acc_ref)
    factor_ref[...] = jnp.zeros_like(factor_ref)
    for g in range(groups):
        weight_refs[g][...] = jnp.zeros_like(weight_refs[g])
        score(loc_ref[0], g)

    def body(t, carry):
        prev = loc_ref[jnp.maximum(t - 1, 0)]
        for g in range(groups):
            apply(prev, g)
            weigh(score_refs[g][...], top_ref[g], g)
            score(loc_ref[t + 1], g)
        return carry

    lax.fori_loop(0, own, body, 0)
    prev = loc_ref[jnp.maximum(own - 1, 0)]
    key_i = lax.broadcasted_iota(jnp.int32, (SPAN, GW), 0)
    col_i = lax.broadcasted_iota(jnp.int32, (SPAN, GW), 1)
    for g in range(groups):
        apply(prev, g)
        r = (col_i + g * GW) & (nrow - 1)
        row_i = (r >> (rows.bit_length() - 1)) * run + part * rows + (r & (rows - 1))
        s = jnp.where(key_i <= row_i, score_refs[g][...], MASKED)
        weigh(s, jnp.max(s.reshape(SPAN // 8, 8, GW), axis=0), g)
    for g in range(groups):
        apply(loc_ref[own], g)
    for g in range(groups):
        total = jnp.sum(sum_ref[g], axis=0, keepdims=True)
        done = (acc_ref[g].reshape(HD, GW) * (1.0 / total)).T.astype(jnp.bfloat16)
        n = min(nrow, GW)
        for c in range(0, GW, n):
            h, r0 = divmod(g * GW + c, nrow)
            out_ref[r0 // rows:(r0 + n) // rows, :, h * HD:(h + 1) * HD] = done[c:c + n].reshape(n // rows, rows, HD)


def attend(own, loc, core, queries, first, second, part, tp_count):
    tok, width = queries.shape
    heads = width // HD
    run = tok // tp_count
    rows = run // PARTS
    spans = tok // SPAN
    per = tp_count // spans
    slots = first.shape[0]
    keys = slots * tok
    groups = per * rows * heads // GW
    pairs = heads * rows * per * spans * keys
    return pl.pallas_call(
        functools.partial(attend_kernel, rows=rows, part=part, heads=heads, run=run),
        out_shape=jax.ShapeDtypeStruct((tp_count, rows, width), jnp.bfloat16),
        grid_spec=pltpu.PrefetchScalarGridSpec(
            num_scalar_prefetch=3,
            grid=(spans,),
            in_specs=[
                pl.BlockSpec((per, rows, width), lambda s, *_: (s, part, 0)),
                VMEM_SPEC,
                VMEM_SPEC,
            ],
            out_specs=pl.BlockSpec((per, rows, width), lambda s, *_: (s, 0, 0)),
            scratch_shapes=[
                pltpu.VMEM((keys, HD), jnp.bfloat16),
                pltpu.VMEM((keys // SPAN, HD, SPAN), jnp.bfloat16),
                pltpu.VMEM((HD, per * rows * heads), jnp.bfloat16),
                pltpu.VMEM((groups, HD // 8, 8, GW), jnp.float32),
                pltpu.VMEM((groups, 8, GW), jnp.float32),
                pltpu.VMEM((groups, 8, GW), jnp.float32),
                pltpu.VMEM((groups, 8, GW), jnp.float32),
                pltpu.VMEM((groups, 8, GW), jnp.float32),
            ]
            + [pltpu.VMEM((SPAN, GW), jnp.float32)] * groups
            + [pltpu.VMEM((SPAN, GW), jnp.bfloat16)] * groups,
        ),
        compiler_params=pltpu.CompilerParams(dimension_semantics=("arbitrary",), vmem_limit_bytes=20 * 2**20),
        cost_estimate=pl.CostEstimate(flops=8 * HD * pairs, bytes_accessed=4 * keys * HD, transcendentals=pairs),
    )(own, loc, core, queries.reshape(tp_count, run, width), first, second)


def stack_kernel(*refs):
    for i, x in enumerate(refs[:-1]):
        refs[-1][i] = x[...]


def stacked(pieces):
    return pl.pallas_call(
        stack_kernel,
        out_shape=jax.ShapeDtypeStruct((len(pieces), *pieces[0].shape), pieces[0].dtype),
        in_specs=[VMEM_SPEC] * len(pieces),
        out_specs=VMEM_SPEC,
        compiler_params=pltpu.CompilerParams(vmem_limit_bytes=8 * 2**20),
    )(*pieces)


def project_kernel(place_ref, *refs):
    atts, near, far, (acc_ref,), outs = refs[:4], refs[4:6], refs[6:10], refs[14:], refs[10:14]
    step = pl.program_id(0)
    rows, k = acc_ref.shape[0], atts[0].shape[-1]
    near_term = jnp.dot(atts[0][...].reshape(rows, k), near[0][...], preferred_element_type=jnp.float32)
    near_term += jnp.dot(atts[1][...].reshape(rows, k), near[1][...], preferred_element_type=jnp.float32)
    for j, w in enumerate(far):
        @pl.when(step == j)
        def _(w=w):
            total = near_term + jnp.dot(atts[2][...].reshape(rows, k), w[0], preferred_element_type=jnp.float32)
            acc_ref[...] = total + jnp.dot(atts[3][...].reshape(rows, k), w[1], preferred_element_type=jnp.float32)
    n = outs[0].shape[0]
    for i, o in enumerate(outs):
        o[...] = acc_ref[pl.ds(pl.multiple_of((place_ref[1] ^ i) * n, n), n), :].astype(jnp.bfloat16)


def project(place, atts, kept, paired, far):
    tps, r, k = atts[0].shape
    rows, cut = tps * r, far[0].shape[-1]
    blocks = len(far)
    col = lambda j, p: (p[2] - j) & (blocks - 1)
    return pl.pallas_call(
        project_kernel,
        out_shape=[jax.ShapeDtypeStruct((rows // 4, cut * blocks), jnp.bfloat16)] * 4,
        grid_spec=pltpu.PrefetchScalarGridSpec(
            num_scalar_prefetch=1,
            grid=(blocks,),
            in_specs=[VMEM_SPEC] * 4
            + [pl.BlockSpec((k, cut), lambda j, p: (0, col(j, p)))] * 2
            + [VMEM_SPEC] * blocks,
            out_specs=[pl.BlockSpec((rows // 4, cut), lambda j, p: (0, col(j, p)))] * 4,
            scratch_shapes=[pltpu.VMEM((rows, cut), jnp.float32)],
        ),
        compiler_params=pltpu.CompilerParams(dimension_semantics=("arbitrary",), vmem_limit_bytes=20 * 2**20),
        cost_estimate=pl.CostEstimate(flops=8 * rows * k * cut * blocks, bytes_accessed=8 * k * cut * blocks, transcendentals=0),
        name="project",
    )(place, *atts, kept, paired, *far)


def add_kernel(m_ref, *refs):
    ins, outs = refs[:4], refs[4:]
    r = outs[0].shape[0]
    for i, o in enumerate(outs):
        rows = pl.ds(pl.multiple_of((m_ref[0] ^ i) * r, r), r)
        total = ins[0][rows, :].astype(jnp.float32)
        for x in ins[1:]:
            total = total + x[rows, :].astype(jnp.float32)
        o[...] = total.astype(jnp.bfloat16)


def add_parts(member, parts):
    rows, n = parts[0].shape
    return pl.pallas_call(
        add_kernel,
        out_shape=[jax.ShapeDtypeStruct((rows // 4, n), jnp.bfloat16)] * 4,
        in_specs=[pl.BlockSpec(memory_space=pltpu.SMEM)] + [VMEM_SPEC] * 4,
        out_specs=[VMEM_SPEC] * 4,
        compiler_params=pltpu.CompilerParams(vmem_limit_bytes=8 * 2**20),
        cost_estimate=pl.CostEstimate(flops=4 * rows * n, bytes_accessed=10 * rows * n, transcendentals=0),
        name="add_parts",
    )(member, *parts)


def finish_kernel(m_ref, scale_ref, res_ref, gain_ref, *refs):
    parts, (hidden_ref, clipped_ref, tmp_ref) = refs[:4], refs[4:]
    n = parts[0].shape[1]
    square = None
    for i, part in enumerate(parts):
        cols = pl.ds(pl.multiple_of((m_ref[0] ^ i) * n, n), n)
        s = res_ref[:, cols].astype(jnp.float32) + part[...].astype(jnp.float32)
        tmp_ref[:, cols] = s
        hidden_ref[:, cols] = s.astype(jnp.bfloat16)
        t = jnp.sum(s * s, axis=1, keepdims=True)
        square = t if square is None else square + t
    inv = lax.rsqrt(square / (4 * n) + 1e-05)
    limit = 448.0 * scale_ref[0]
    clipped_ref[...] = jnp.clip(tmp_ref[...] * inv * gain_ref[...], -limit, limit).astype(jnp.bfloat16)


def finish(member, static_scale, residual, gain, parts, part, before):
    rows, width = residual.shape
    r = rows // PARTS
    whole = pl.BlockSpec((r, width), lambda i, *_: (part, 0))
    kernel = finish_kernel
    if before:
        kernel = lambda m, s, res, g, a, b, c, d, e, f, *rest: finish_kernel(m, s, res, g, a, b, c, d, *rest)
    return pl.pallas_call(
        kernel,
        out_shape=[jax.ShapeDtypeStruct((rows, width), jnp.bfloat16)] * 2,
        grid_spec=pltpu.PrefetchScalarGridSpec(
            num_scalar_prefetch=2,
            grid=(1,),
            in_specs=[whole, pl.BlockSpec((1, width), lambda i, *_: (0, 0))]
            + [VMEM_SPEC] * 4
            + [pl.BlockSpec(memory_space=ANY)] * len(before),
            out_specs=[whole] * 2,
            scratch_shapes=[pltpu.VMEM((r, width), jnp.float32)],
        ),
        input_output_aliases={8 + i: i for i in range(len(before))},
        compiler_params=pltpu.CompilerParams(vmem_limit_bytes=12 * 2**20),
        cost_estimate=pl.CostEstimate(flops=8 * r * width, bytes_accessed=10 * r * width, transcendentals=0),
    )(member, static_scale, residual, gain, *parts, *before)


def swapped(value, mask, count):
    return lax.ppermute(value, "tp", [(i, i ^ mask) for i in range(count)])


def shards(
    queries,
    context_keys,
    context_values,
    positions,
    out_weight,
    residual_in,
    norm_gain,
    static_scale,
):
    ctx_count = lax.axis_size("ctx")
    tp_count = lax.axis_size("tp")
    tp_rank = lax.axis_index("tp").astype(jnp.int32)
    tok, _ = queries.shape
    core = tp_rank & 1
    member = tp_rank & 3
    group = tp_rank >> 2
    y_rank = lax.axis_index("ctx").astype(jnp.int32) & (Y_COUNT - 1)

    kv_col = (tp_rank >> 1) * HD
    mine = jnp.where(
        core == 0,
        lax.dynamic_slice_in_dim(context_keys, kv_col, HD, 1),
        lax.dynamic_slice_in_dim(context_values, kv_col, HD, 1),
    )
    spans = tok // SPAN
    own = positions[::SPAN] // SPAN
    tag = jnp.pad(own.astype(jnp.bfloat16)[:, None] * jnp.ones((1, HD), jnp.bfloat16), ((0, 16 - spans), (0, 0)))
    mine = jnp.concatenate([mine, tag], axis=0)
    pieces = [mine]
    for dz in range(ctx_count // Y_COUNT):
        for dy in (0, 2, 1, 3):
            if dz or dy:
                pairs = [
                    (c, (c // Y_COUNT ^ dz) * Y_COUNT + (c + dy) % Y_COUNT) for c in range(ctx_count)
                ]
                pieces.append(lax.ppermute(mine, "ctx", pairs))
    first = stacked(pieces)
    second = swapped(first, 1, tp_count)
    order = first[:, tok:tok + spans, 0].reshape(ctx_count * spans).astype(jnp.int32)
    blocks = jnp.arange(ctx_count * spans, dtype=jnp.int32)
    loc = jnp.sum(jnp.where(order[None, :] == blocks[:, None], blocks[None, :], 0), axis=1)

    quarter = out_weight.shape[1] // 4
    cut = quarter // Y_COUNT
    sides = []
    for i in (2, 3):
        w = lax.dynamic_slice_in_dim(out_weight, (member ^ i) * quarter + y_rank * cut, cut, 1)
        sides.append(swapped(w, i, tp_count))
    side = stacked(sides)
    far = [side]
    for dy in (1, 2, 3):
        pairs = [(c, c - c % Y_COUNT + (c + dy) % Y_COUNT) for c in range(ctx_count)]
        far.append(lax.ppermute(side, "ctx", pairs))
    kept, w = (lax.dynamic_slice_in_dim(out_weight, (member ^ i) * quarter, quarter, 1) for i in (0, 1))
    paired = swapped(w, 1, tp_count)
    place = jnp.stack([member, group, y_rank])

    outs = ()
    for part in range(PARTS):
        att = attend(own, loc, core[None], queries, first, second, part, tp_count)
        atts = [att]
        for i in (1, 2, 3):
            atts.append(swapped(att, i, tp_count))
        sent = project(place, atts, kept, paired, far)
        got = [sent[0]]
        for i in (1, 2, 3):
            got.append(swapped(sent[i], 4 * i, tp_count))
        cols = list(add_parts(member[None], got))
        for i in (1, 2, 3):
            cols[i] = swapped(cols[i], i, tp_count)
        outs = finish(member[None], static_scale, residual_in, norm_gain[None, :], cols, part, outs)
    return tuple(outs)


def solution(mesh):
    return jax.shard_map(
        shards,
        mesh=mesh,
        in_specs=(
            P("ctx", "tp"),
            P("ctx", None),
            P("ctx", None),
            P("ctx"),
            P("tp", None),
            P(("ctx", "tp"), None),
            P(),
            P(),
        ),
        out_specs=(P(("ctx", "tp"), None), P(("ctx", "tp"), None)),
        check_vma=False,
    )
```

```python
import functools
import math

import jax
import jax.numpy as jnp
from jax import lax
from jax.experimental import pallas as pl
from jax.experimental.pallas import tpu as pltpu
from jax.sharding import PartitionSpec as P


HD = 128
SPAN = 512
GW = 256
MASKED = -1e30
LOG2_SCALE = math.log2(math.e) / math.sqrt(HD)
PARTS = 2
Y_COUNT = 4
ANY = pl.ANY
VMEM_SPEC = pl.BlockSpec(memory_space=pltpu.VMEM)


def attend_kernel(
    own_ref, loc_ref, core_ref, q_ref, first_ref, second_ref, out_ref,
    k_ref, vt_ref, qt_ref, acc_ref, max_ref, sum_ref, top_ref, factor_ref, *tile_refs,
    rows, part, heads, run,
):
    span = pl.program_id(0)
    slots = first_ref.shape[0]
    block_rows = k_ref.shape[0] // slots
    nrow = q_ref.shape[0] * rows
    groups = nrow * heads // GW
    score_refs, weight_refs = tile_refs[:groups], tile_refs[groups:]

    @pl.when(span == 0)
    def _():
        def take(keys, values):
            for i in range(slots):
                at = i * block_rows
                k_ref[at:at + block_rows, :] = keys[i, :block_rows, :]
                for b in range(0, block_rows, SPAN):
                    vt_ref[(at + b) // SPAN] = values[i, b:b + SPAN, :].T

        @pl.when(core_ref[0] == 0)
        def _():
            take(first_ref, second_ref)

        @pl.when(core_ref[0] != 0)
        def _():
            take(second_ref, first_ref)

    own = own_ref[span]
    q_all = q_ref[...].reshape(nrow, heads * HD)
    for h in range(heads):
        qt_ref[:, h * nrow:(h + 1) * nrow] = q_all[:, h * HD:(h + 1) * HD].T

    def score(blk, g):
        keys = k_ref[pl.ds(pl.multiple_of(blk * SPAN, SPAN), SPAN), :]
        s = jnp.dot(keys, qt_ref[:, g * GW:(g + 1) * GW], preferred_element_type=jnp.float32)
        score_refs[g][...] = s
        top_ref[g] = jnp.max(s.reshape(SPAN // 8, 8, GW), axis=0)

    def weigh(s, top, g):
        old = max_ref[g]
        new = jnp.maximum(old, jnp.broadcast_to(jnp.max(top, axis=0, keepdims=True), old.shape))
        max_ref[g] = new
        p = jnp.exp2(s.reshape(SPAN // 8, 8, GW) * LOG2_SCALE - (new * LOG2_SCALE)[None])
        factor = jnp.exp2((old - new) * LOG2_SCALE)
        factor_ref[g] = factor
        sum_ref[g] = sum_ref[g] * factor + jnp.sum(p, axis=0)
        weight_refs[g][...] = p.reshape(SPAN, GW).astype(jnp.bfloat16)

    def apply(blk, g):
        pv = jnp.dot(vt_ref[blk], weight_refs[g][...], preferred_element_type=jnp.float32)
        acc_ref[g] = acc_ref[g] * factor_ref[g][None] + pv.reshape(HD // 8, 8, GW)

    max_ref[...] = jnp.full_like(max_ref, MASKED)
    sum_ref[...] = jnp.zeros_like(sum_ref)
    acc_ref[...] = jnp.zeros_like(acc_ref)
    factor_ref[...] = jnp.zeros_like(factor_ref)
    for g in range(groups):
        weight_refs[g][...] = jnp.zeros_like(weight_refs[g])
        score(loc_ref[0], g)

    def body(t, carry):
        prev = loc_ref[jnp.maximum(t - 1, 0)]
        for g in range(groups):
            apply(prev, g)
            weigh(score_refs[g][...], top_ref[g], g)
            score(loc_ref[t + 1], g)
        return carry

    lax.fori_loop(0, own, body, 0)
    prev = loc_ref[jnp.maximum(own - 1, 0)]
    key_i = lax.broadcasted_iota(jnp.int32, (SPAN, GW), 0)
    col_i = lax.broadcasted_iota(jnp.int32, (SPAN, GW), 1)
    for g in range(groups):
        apply(prev, g)
        r = (col_i + g * GW) & (nrow - 1)
        row_i = (r >> (rows.bit_length() - 1)) * run + part * rows + (r & (rows - 1))
        s = jnp.where(key_i <= row_i, score_refs[g][...], MASKED)
        weigh(s, jnp.max(s.reshape(SPAN // 8, 8, GW), axis=0), g)
    for g in range(groups):
        apply(loc_ref[own], g)
    for g in range(groups):
        total = jnp.sum(sum_ref[g], axis=0, keepdims=True)
        done = (acc_ref[g].reshape(HD, GW) * (1.0 / total)).T.astype(jnp.bfloat16)
        n = min(nrow, GW)
        for c in range(0, GW, n):
            h, r0 = divmod(g * GW + c, nrow)
            out_ref[r0 // rows:(r0 + n) // rows, :, h * HD:(h + 1) * HD] = done[c:c + n].reshape(n // rows, rows, HD)


def attend(own, loc, core, queries, first, second, part, tp_count):
    tok, width = queries.shape
    heads = width // HD
    run = tok // tp_count
    rows = run // PARTS
    spans = tok // SPAN
    per = tp_count // spans
    slots = first.shape[0]
    keys = slots * tok
    groups = per * rows * heads // GW
    pairs = heads * rows * per * spans * keys
    return pl.pallas_call(
        functools.partial(attend_kernel, rows=rows, part=part, heads=heads, run=run),
        out_shape=jax.ShapeDtypeStruct((tp_count, rows, width), jnp.bfloat16),
        grid_spec=pltpu.PrefetchScalarGridSpec(
            num_scalar_prefetch=3,
            grid=(spans,),
            in_specs=[
                pl.BlockSpec((per, rows, width), lambda s, *_: (s, part, 0)),
                VMEM_SPEC,
                VMEM_SPEC,
            ],
            out_specs=pl.BlockSpec((per, rows, width), lambda s, *_: (s, 0, 0)),
            scratch_shapes=[
                pltpu.VMEM((keys, HD), jnp.bfloat16),
                pltpu.VMEM((keys // SPAN, HD, SPAN), jnp.bfloat16),
                pltpu.VMEM((HD, per * rows * heads), jnp.bfloat16),
                pltpu.VMEM((groups, HD // 8, 8, GW), jnp.float32),
                pltpu.VMEM((groups, 8, GW), jnp.float32),
                pltpu.VMEM((groups, 8, GW), jnp.float32),
                pltpu.VMEM((groups, 8, GW), jnp.float32),
                pltpu.VMEM((groups, 8, GW), jnp.float32),
            ]
            + [pltpu.VMEM((SPAN, GW), jnp.float32)] * groups
            + [pltpu.VMEM((SPAN, GW), jnp.bfloat16)] * groups,
        ),
        compiler_params=pltpu.CompilerParams(dimension_semantics=("arbitrary",), vmem_limit_bytes=20 * 2**20),
        cost_estimate=pl.CostEstimate(flops=8 * HD * pairs, bytes_accessed=4 * keys * HD, transcendentals=pairs),
    )(own, loc, core, queries.reshape(tp_count, run, width), first, second)


def stack_kernel(*refs):
    ins, out_ref, sems = refs[:-2], refs[-2], refs[-1]
    copies = [pltpu.make_async_copy(x, out_ref.at[i], sems.at[i]) for i, x in enumerate(ins)]
    for c in copies:
        c.start()
    for c in copies:
        c.wait()


def stacked(pieces):
    return pl.pallas_call(
        stack_kernel,
        out_shape=jax.ShapeDtypeStruct((len(pieces), *pieces[0].shape), pieces[0].dtype),
        in_specs=[pl.BlockSpec(memory_space=ANY)] * len(pieces),
        out_specs=VMEM_SPEC,
        scratch_shapes=[pltpu.SemaphoreType.DMA((len(pieces),))],
        compiler_params=pltpu.CompilerParams(vmem_limit_bytes=57 * 2**20),
    )(*pieces)


def project_kernel(place_ref, *refs):
    atts, near, far, (acc_ref,), outs = refs[:4], refs[4:6], refs[6:10], refs[14:], refs[10:14]
    step = pl.program_id(0)
    rows, k = acc_ref.shape[0], atts[0].shape[-1]
    near_term = jnp.dot(atts[0][...].reshape(rows, k), near[0][...], preferred_element_type=jnp.float32)
    near_term += jnp.dot(atts[1][...].reshape(rows, k), near[1][...], preferred_element_type=jnp.float32)
    for j, w in enumerate(far):
        @pl.when(step == j)
        def _(w=w):
            total = near_term + jnp.dot(atts[2][...].reshape(rows, k), w[0], preferred_element_type=jnp.float32)
            acc_ref[...] = total + jnp.dot(atts[3][...].reshape(rows, k), w[1], preferred_element_type=jnp.float32)
    n = outs[0].shape[0]
    for i, o in enumerate(outs):
        o[...] = acc_ref[pl.ds(pl.multiple_of((place_ref[1] ^ i) * n, n), n), :].astype(jnp.bfloat16)


def project(place, atts, kept, paired, far):
    tps, r, k = atts[0].shape
    rows, cut = tps * r, far[0].shape[-1]
    blocks = len(far)
    col = lambda j, p: (p[2] - j) & (blocks - 1)
    return pl.pallas_call(
        project_kernel,
        out_shape=[jax.ShapeDtypeStruct((rows // 4, cut * blocks), jnp.bfloat16)] * 4,
        grid_spec=pltpu.PrefetchScalarGridSpec(
            num_scalar_prefetch=1,
            grid=(blocks,),
            in_specs=[VMEM_SPEC] * 4
            + [pl.BlockSpec((k, cut), lambda j, p: (0, col(j, p)))] * 2
            + [VMEM_SPEC] * blocks,
            out_specs=[pl.BlockSpec((rows // 4, cut), lambda j, p: (0, col(j, p)))] * 4,
            scratch_shapes=[pltpu.VMEM((rows, cut), jnp.float32)],
        ),
        compiler_params=pltpu.CompilerParams(dimension_semantics=("arbitrary",), vmem_limit_bytes=20 * 2**20),
        cost_estimate=pl.CostEstimate(flops=8 * rows * k * cut * blocks, bytes_accessed=8 * k * cut * blocks, transcendentals=0),
        name="project",
    )(place, *atts, kept, paired, *far)


def add_kernel(m_ref, *refs):
    ins, outs = refs[:4], refs[4:]
    r = outs[0].shape[0]
    for i, o in enumerate(outs):
        rows = pl.ds(pl.multiple_of((m_ref[0] ^ i) * r, r), r)
        total = ins[0][rows, :].astype(jnp.float32)
        for x in ins[1:]:
            total = total + x[rows, :].astype(jnp.float32)
        o[...] = total.astype(jnp.bfloat16)


def add_parts(member, parts):
    rows, n = parts[0].shape
    return pl.pallas_call(
        add_kernel,
        out_shape=[jax.ShapeDtypeStruct((rows // 4, n), jnp.bfloat16)] * 4,
        in_specs=[pl.BlockSpec(memory_space=pltpu.SMEM)] + [VMEM_SPEC] * 4,
        out_specs=[VMEM_SPEC] * 4,
        compiler_params=pltpu.CompilerParams(vmem_limit_bytes=8 * 2**20),
        cost_estimate=pl.CostEstimate(flops=4 * rows * n, bytes_accessed=10 * rows * n, transcendentals=0),
        name="add_parts",
    )(member, *parts)


def finish_kernel(m_ref, scale_ref, res_ref, gain_ref, *refs):
    parts, (hidden_ref, clipped_ref, tmp_ref) = refs[:4], refs[4:]
    n = parts[0].shape[1]
    square = None
    for i, part in enumerate(parts):
        cols = pl.ds(pl.multiple_of((m_ref[0] ^ i) * n, n), n)
        s = res_ref[:, cols].astype(jnp.float32) + part[...].astype(jnp.float32)
        tmp_ref[:, cols] = s
        hidden_ref[:, cols] = s.astype(jnp.bfloat16)
        t = jnp.sum(s * s, axis=1, keepdims=True)
        square = t if square is None else square + t
    inv = lax.rsqrt(square / (4 * n) + 1e-05)
    limit = 448.0 * scale_ref[0]
    clipped_ref[...] = jnp.clip(tmp_ref[...] * inv * gain_ref[...], -limit, limit).astype(jnp.bfloat16)


def finish(member, static_scale, residual, gain, parts, part, before):
    rows, width = residual.shape
    r = rows // PARTS
    whole = pl.BlockSpec((r, width), lambda i, *_: (part, 0))
    kernel = finish_kernel
    if before:
        kernel = lambda m, s, res, g, a, b, c, d, e, f, *rest: finish_kernel(m, s, res, g, a, b, c, d, *rest)
    return pl.pallas_call(
        kernel,
        out_shape=[jax.ShapeDtypeStruct((rows, width), jnp.bfloat16)] * 2,
        grid_spec=pltpu.PrefetchScalarGridSpec(
            num_scalar_prefetch=2,
            grid=(1,),
            in_specs=[whole, pl.BlockSpec((1, width), lambda i, *_: (0, 0))]
            + [VMEM_SPEC] * 4
            + [pl.BlockSpec(memory_space=ANY)] * len(before),
            out_specs=[whole] * 2,
            scratch_shapes=[pltpu.VMEM((r, width), jnp.float32)],
        ),
        input_output_aliases={8 + i: i for i in range(len(before))},
        compiler_params=pltpu.CompilerParams(vmem_limit_bytes=12 * 2**20),
        cost_estimate=pl.CostEstimate(flops=8 * r * width, bytes_accessed=10 * r * width, transcendentals=0),
    )(member, static_scale, residual, gain, *parts, *before)


def swapped(value, mask, count):
    return lax.ppermute(value, "tp", [(i, i ^ mask) for i in range(count)])


def shards(
    queries,
    context_keys,
    context_values,
    positions,
    out_weight,
    residual_in,
    norm_gain,
    static_scale,
):
    ctx_count = lax.axis_size("ctx")
    tp_count = lax.axis_size("tp")
    tp_rank = lax.axis_index("tp").astype(jnp.int32)
    tok, _ = queries.shape
    core = tp_rank & 1
    member = tp_rank & 3
    group = tp_rank >> 2
    y_rank = lax.axis_index("ctx").astype(jnp.int32) & (Y_COUNT - 1)

    kv_col = (tp_rank >> 1) * HD
    mine = jnp.where(
        core == 0,
        lax.dynamic_slice_in_dim(context_keys, kv_col, HD, 1),
        lax.dynamic_slice_in_dim(context_values, kv_col, HD, 1),
    )
    spans = tok // SPAN
    own = positions[::SPAN] // SPAN
    tag = jnp.pad(own.astype(jnp.bfloat16)[:, None] * jnp.ones((1, HD), jnp.bfloat16), ((0, 16 - spans), (0, 0)))
    mine = jnp.concatenate([mine, tag], axis=0)
    pieces = [mine]
    for dz in range(ctx_count // Y_COUNT):
        for dy in (0, 2, 1, 3):
            if dz or dy:
                pairs = [
                    (c, (c // Y_COUNT ^ dz) * Y_COUNT + (c + dy) % Y_COUNT) for c in range(ctx_count)
                ]
                pieces.append(lax.ppermute(mine, "ctx", pairs))
    first = stacked(pieces)
    second = swapped(first, 1, tp_count)
    order = first[:, tok:tok + spans, 0].reshape(ctx_count * spans).astype(jnp.int32)
    blocks = jnp.arange(ctx_count * spans, dtype=jnp.int32)
    loc = jnp.sum(jnp.where(order[None, :] == blocks[:, None], blocks[None, :], 0), axis=1)

    quarter = out_weight.shape[1] // 4
    cut = quarter // Y_COUNT
    sides = []
    for i in (2, 3):
        w = lax.dynamic_slice_in_dim(out_weight, (member ^ i) * quarter + y_rank * cut, cut, 1)
        sides.append(swapped(w, i, tp_count))
    side = stacked(sides)
    far = [side]
    for dy in (1, 2, 3):
        pairs = [(c, c - c % Y_COUNT + (c + dy) % Y_COUNT) for c in range(ctx_count)]
        far.append(lax.ppermute(side, "ctx", pairs))
    kept, w = (lax.dynamic_slice_in_dim(out_weight, (member ^ i) * quarter, quarter, 1) for i in (0, 1))
    paired = swapped(w, 1, tp_count)
    place = jnp.stack([member, group, y_rank])

    outs = ()
    for part in range(PARTS):
        att = attend(own, loc, core[None], queries, first, second, part, tp_count)
        atts = [att]
        for source, mask in ((0, 2), (0, 1), (1, 1)):
            atts.append(swapped(atts[source], mask, tp_count))
        atts = [atts[i] for i in (0, 2, 1, 3)]
        sent = project(place, atts, kept, paired, far)
        got = [sent[0]]
        for i in (1, 2, 3):
            got.append(swapped(sent[i], 4 * i, tp_count))
        cols = list(add_parts(member[None], got))
        for i in (1, 2, 3):
            cols[i] = swapped(cols[i], i, tp_count)
        outs = finish(member[None], static_scale, residual_in, norm_gain[None, :], cols, part, outs)
    return tuple(outs)


def solution(mesh):
    return jax.shard_map(
        shards,
        mesh=mesh,
        in_specs=(
            P("ctx", "tp"),
            P("ctx", None),
            P("ctx", None),
            P("ctx"),
            P("tp", None),
            P(("ctx", "tp"), None),
            P(),
            P(),
        ),
        out_specs=(P(("ctx", "tp"), None), P(("ctx", "tp"), None)),
        check_vma=False,
    )
```

```python
import functools
import math

import jax
import jax.numpy as jnp
from jax import lax
from jax.experimental import pallas as pl
from jax.experimental.pallas import tpu as pltpu
from jax.sharding import PartitionSpec as P


HD = 128
SPAN = 512
GW = 256
MASKED = -1e30
LOG2_SCALE = math.log2(math.e) / math.sqrt(HD)
PARTS = 2
Y_COUNT = 4
ANY = pl.ANY
VMEM_SPEC = pl.BlockSpec(memory_space=pltpu.VMEM)


def attend_kernel(
    own_ref, loc_ref, core_ref, q_ref, first_ref, second_ref, out_ref,
    k_ref, vt_ref, qt_ref, acc_ref, max_ref, sum_ref, top_ref, factor_ref, *tile_refs,
    rows, part, heads, run,
):
    span = pl.program_id(0)
    slots = first_ref.shape[0]
    block_rows = k_ref.shape[0] // slots
    nrow = q_ref.shape[0] * rows
    groups = nrow * heads // GW
    score_refs, weight_refs = tile_refs[:groups], tile_refs[groups:]

    @pl.when(span == 0)
    def _():
        def take(keys, values):
            for i in range(slots):
                at = i * block_rows
                k_ref[at:at + block_rows, :] = keys[i, :block_rows, :]
                for b in range(0, block_rows, SPAN):
                    vt_ref[(at + b) // SPAN] = values[i, b:b + SPAN, :].T

        @pl.when(core_ref[0] == 0)
        def _():
            take(first_ref, second_ref)

        @pl.when(core_ref[0] != 0)
        def _():
            take(second_ref, first_ref)

    own = own_ref[span]
    q_all = q_ref[...].reshape(nrow, heads * HD)
    for h in range(heads):
        qt_ref[:, h * nrow:(h + 1) * nrow] = q_all[:, h * HD:(h + 1) * HD].T

    def score(blk, g):
        keys = k_ref[pl.ds(pl.multiple_of(blk * SPAN, SPAN), SPAN), :]
        s = jnp.dot(keys, qt_ref[:, g * GW:(g + 1) * GW], preferred_element_type=jnp.float32)
        score_refs[g][...] = s
        top_ref[g] = jnp.max(s.reshape(SPAN // 8, 8, GW), axis=0)

    def weigh(s, top, g):
        old = max_ref[g]
        new = jnp.maximum(old, jnp.broadcast_to(jnp.max(top, axis=0, keepdims=True), old.shape))
        max_ref[g] = new
        p = jnp.exp2(s.reshape(SPAN // 8, 8, GW) * LOG2_SCALE - (new * LOG2_SCALE)[None])
        factor = jnp.exp2((old - new) * LOG2_SCALE)
        factor_ref[g] = factor
        sum_ref[g] = sum_ref[g] * factor + jnp.sum(p, axis=0)
        weight_refs[g][...] = p.reshape(SPAN, GW).astype(jnp.bfloat16)

    def apply(blk, g):
        pv = jnp.dot(vt_ref[blk], weight_refs[g][...], preferred_element_type=jnp.float32)
        acc_ref[g] = acc_ref[g] * factor_ref[g][None] + pv.reshape(HD // 8, 8, GW)

    max_ref[...] = jnp.full_like(max_ref, MASKED)
    sum_ref[...] = jnp.zeros_like(sum_ref)
    acc_ref[...] = jnp.zeros_like(acc_ref)
    factor_ref[...] = jnp.zeros_like(factor_ref)
    for g in range(groups):
        weight_refs[g][...] = jnp.zeros_like(weight_refs[g])
        score(loc_ref[0], g)

    def body(t, carry):
        prev = loc_ref[jnp.maximum(t - 1, 0)]
        for g in range(groups):
            apply(prev, g)
            weigh(score_refs[g][...], top_ref[g], g)
            score(loc_ref[t + 1], g)
        return carry

    lax.fori_loop(0, own, body, 0)
    prev = loc_ref[jnp.maximum(own - 1, 0)]
    key_i = lax.broadcasted_iota(jnp.int32, (SPAN, GW), 0)
    col_i = lax.broadcasted_iota(jnp.int32, (SPAN, GW), 1)
    for g in range(groups):
        apply(prev, g)
        r = (col_i + g * GW) & (nrow - 1)
        row_i = (r >> (rows.bit_length() - 1)) * run + part * rows + (r & (rows - 1))
        s = jnp.where(key_i <= row_i, score_refs[g][...], MASKED)
        weigh(s, jnp.max(s.reshape(SPAN // 8, 8, GW), axis=0), g)
    for g in range(groups):
        apply(loc_ref[own], g)
    for g in range(groups):
        total = jnp.sum(sum_ref[g], axis=0, keepdims=True)
        done = (acc_ref[g].reshape(HD, GW) * (1.0 / total)).T.astype(jnp.bfloat16)
        n = min(nrow, GW)
        for c in range(0, GW, n):
            h, r0 = divmod(g * GW + c, nrow)
            out_ref[r0 // rows:(r0 + n) // rows, :, h * HD:(h + 1) * HD] = done[c:c + n].reshape(n // rows, rows, HD)


def attend(own, loc, core, queries, first, second, part, tp_count):
    tok, width = queries.shape
    heads = width // HD
    run = tok // tp_count
    rows = run // PARTS
    spans = tok // SPAN
    per = tp_count // spans
    slots = first.shape[0]
    keys = slots * tok
    groups = per * rows * heads // GW
    pairs = heads * rows * per * spans * keys
    return pl.pallas_call(
        functools.partial(attend_kernel, rows=rows, part=part, heads=heads, run=run),
        out_shape=jax.ShapeDtypeStruct((tp_count, rows, width), jnp.bfloat16),
        grid_spec=pltpu.PrefetchScalarGridSpec(
            num_scalar_prefetch=3,
            grid=(spans,),
            in_specs=[
                pl.BlockSpec((per, rows, width), lambda s, *_: (s, part, 0)),
                VMEM_SPEC,
                VMEM_SPEC,
            ],
            out_specs=pl.BlockSpec((per, rows, width), lambda s, *_: (s, 0, 0)),
            scratch_shapes=[
                pltpu.VMEM((keys, HD), jnp.bfloat16),
                pltpu.VMEM((keys // SPAN, HD, SPAN), jnp.bfloat16),
                pltpu.VMEM((HD, per * rows * heads), jnp.bfloat16),
                pltpu.VMEM((groups, HD // 8, 8, GW), jnp.float32),
                pltpu.VMEM((groups, 8, GW), jnp.float32),
                pltpu.VMEM((groups, 8, GW), jnp.float32),
                pltpu.VMEM((groups, 8, GW), jnp.float32),
                pltpu.VMEM((groups, 8, GW), jnp.float32),
            ]
            + [pltpu.VMEM((SPAN, GW), jnp.float32)] * groups
            + [pltpu.VMEM((SPAN, GW), jnp.bfloat16)] * groups,
        ),
        compiler_params=pltpu.CompilerParams(dimension_semantics=("arbitrary",), vmem_limit_bytes=20 * 2**20),
        cost_estimate=pl.CostEstimate(flops=8 * HD * pairs, bytes_accessed=4 * keys * HD, transcendentals=pairs),
    )(own, loc, core, queries.reshape(tp_count, run, width), first, second)


def stack_kernel(*refs):
    ins, out_ref, sems = refs[:-2], refs[-2], refs[-1]
    copies = [pltpu.make_async_copy(x, out_ref.at[i], sems.at[i]) for i, x in enumerate(ins)]
    for c in copies:
        c.start()
    for c in copies:
        c.wait()


def stacked(pieces):
    return pl.pallas_call(
        stack_kernel,
        out_shape=jax.ShapeDtypeStruct((len(pieces), *pieces[0].shape), pieces[0].dtype),
        in_specs=[pl.BlockSpec(memory_space=ANY)] * len(pieces),
        out_specs=VMEM_SPEC,
        scratch_shapes=[pltpu.SemaphoreType.DMA((len(pieces),))],
        compiler_params=pltpu.CompilerParams(vmem_limit_bytes=57 * 2**20),
    )(*pieces)


def project_kernel(place_ref, *refs):
    atts, near, far, outs, acc_ref = refs[:4], refs[4:6], refs[6:10], refs[10:14], refs[14]
    rows, cut = acc_ref.shape
    n = outs[0].shape[0]
    for j, w in enumerate(far):
        cols = pl.ds(pl.multiple_of(((place_ref[2] - j) & (len(far) - 1)) * cut, cut), cut)
        total = None
        for m, a in enumerate(atts):
            weight = near[m][:, cols] if m < 2 else w[m - 2]
            term = jnp.dot(a[...].reshape(rows, a.shape[-1]), weight, preferred_element_type=jnp.float32)
            total = term if total is None else total + term
        acc_ref[...] = total
        for i, o in enumerate(outs):
            o[:, cols] = acc_ref[pl.ds(pl.multiple_of((place_ref[1] ^ i) * n, n), n), :].astype(jnp.bfloat16)


def project(place, atts, kept, paired, far):
    tps, r, k = atts[0].shape
    rows, cut = tps * r, far[0].shape[-1]
    n = cut * len(far)
    return pl.pallas_call(
        project_kernel,
        out_shape=[jax.ShapeDtypeStruct((rows // 4, n), jnp.bfloat16)] * 4,
        in_specs=[pl.BlockSpec(memory_space=pltpu.SMEM)] + [VMEM_SPEC] * (6 + len(far)),
        out_specs=[VMEM_SPEC] * 4,
        scratch_shapes=[pltpu.VMEM((rows, cut), jnp.float32)],
        compiler_params=pltpu.CompilerParams(vmem_limit_bytes=16 * 2**20),
        cost_estimate=pl.CostEstimate(flops=8 * rows * k * n, bytes_accessed=8 * k * n, transcendentals=0),
        name="project",
    )(place, *atts, kept, paired, *far)


def add_kernel(m_ref, *refs):
    ins, outs = refs[:4], refs[4:]
    r = outs[0].shape[0]
    for i, o in enumerate(outs):
        rows = pl.ds(pl.multiple_of((m_ref[0] ^ i) * r, r), r)
        total = ins[0][rows, :].astype(jnp.float32)
        for x in ins[1:]:
            total = total + x[rows, :].astype(jnp.float32)
        o[...] = total.astype(jnp.bfloat16)


def add_parts(member, parts):
    rows, n = parts[0].shape
    return pl.pallas_call(
        add_kernel,
        out_shape=[jax.ShapeDtypeStruct((rows // 4, n), jnp.bfloat16)] * 4,
        in_specs=[pl.BlockSpec(memory_space=pltpu.SMEM)] + [VMEM_SPEC] * 4,
        out_specs=[VMEM_SPEC] * 4,
        compiler_params=pltpu.CompilerParams(vmem_limit_bytes=8 * 2**20),
        cost_estimate=pl.CostEstimate(flops=4 * rows * n, bytes_accessed=10 * rows * n, transcendentals=0),
        name="add_parts",
    )(member, *parts)


def finish_kernel(m_ref, scale_ref, res_ref, gain_ref, *refs):
    parts, (hidden_ref, clipped_ref, tmp_ref) = refs[:4], refs[4:]
    n = parts[0].shape[1]
    square = None
    for i, part in enumerate(parts):
        cols = pl.ds(pl.multiple_of((m_ref[0] ^ i) * n, n), n)
        s = res_ref[:, cols].astype(jnp.float32) + part[...].astype(jnp.float32)
        tmp_ref[:, cols] = s
        hidden_ref[:, cols] = s.astype(jnp.bfloat16)
        t = jnp.sum(s * s, axis=1, keepdims=True)
        square = t if square is None else square + t
    inv = lax.rsqrt(square / (4 * n) + 1e-05)
    limit = 448.0 * scale_ref[0]
    clipped_ref[...] = jnp.clip(tmp_ref[...] * inv * gain_ref[...], -limit, limit).astype(jnp.bfloat16)


def finish(member, static_scale, residual, gain, parts, part, before):
    rows, width = residual.shape
    r = rows // PARTS
    whole = pl.BlockSpec((r, width), lambda i, *_: (part, 0))
    kernel = finish_kernel
    if before:
        kernel = lambda m, s, res, g, a, b, c, d, e, f, *rest: finish_kernel(m, s, res, g, a, b, c, d, *rest)
    return pl.pallas_call(
        kernel,
        out_shape=[jax.ShapeDtypeStruct((rows, width), jnp.bfloat16)] * 2,
        grid_spec=pltpu.PrefetchScalarGridSpec(
            num_scalar_prefetch=2,
            grid=(1,),
            in_specs=[whole, pl.BlockSpec((1, width), lambda i, *_: (0, 0))]
            + [VMEM_SPEC] * 4
            + [pl.BlockSpec(memory_space=ANY)] * len(before),
            out_specs=[whole] * 2,
            scratch_shapes=[pltpu.VMEM((r, width), jnp.float32)],
        ),
        input_output_aliases={8 + i: i for i in range(len(before))},
        compiler_params=pltpu.CompilerParams(vmem_limit_bytes=12 * 2**20),
        cost_estimate=pl.CostEstimate(flops=8 * r * width, bytes_accessed=10 * r * width, transcendentals=0),
    )(member, static_scale, residual, gain, *parts, *before)


def swapped(value, mask, count):
    return lax.ppermute(value, "tp", [(i, i ^ mask) for i in range(count)])


def shards(
    queries,
    context_keys,
    context_values,
    positions,
    out_weight,
    residual_in,
    norm_gain,
    static_scale,
):
    ctx_count = lax.axis_size("ctx")
    tp_count = lax.axis_size("tp")
    tp_rank = lax.axis_index("tp").astype(jnp.int32)
    tok, _ = queries.shape
    core = tp_rank & 1
    member = tp_rank & 3
    group = tp_rank >> 2
    y_rank = lax.axis_index("ctx").astype(jnp.int32) & (Y_COUNT - 1)

    kv_col = (tp_rank >> 1) * HD
    mine = jnp.where(
        core == 0,
        lax.dynamic_slice_in_dim(context_keys, kv_col, HD, 1),
        lax.dynamic_slice_in_dim(context_values, kv_col, HD, 1),
    )
    spans = tok // SPAN
    own = positions[::SPAN] // SPAN
    tag = jnp.pad(own.astype(jnp.bfloat16)[:, None] * jnp.ones((1, HD), jnp.bfloat16), ((0, 16 - spans), (0, 0)))
    mine = jnp.concatenate([mine, tag], axis=0)
    pieces = [mine]
    for dz in range(ctx_count // Y_COUNT):
        for dy in (0, 2, 1, 3):
            if dz or dy:
                pairs = [
                    (c, (c // Y_COUNT ^ dz) * Y_COUNT + (c + dy) % Y_COUNT) for c in range(ctx_count)
                ]
                pieces.append(lax.ppermute(mine, "ctx", pairs))
    first = stacked(pieces)
    second = swapped(first, 1, tp_count)
    order = first[:, tok:tok + spans, 0].reshape(ctx_count * spans).astype(jnp.int32)
    blocks = jnp.arange(ctx_count * spans, dtype=jnp.int32)
    loc = jnp.sum(jnp.where(order[None, :] == blocks[:, None], blocks[None, :], 0), axis=1)

    quarter = out_weight.shape[1] // 4
    cut = quarter // Y_COUNT
    sides = []
    for i in (2, 3):
        w = lax.dynamic_slice_in_dim(out_weight, (member ^ i) * quarter + y_rank * cut, cut, 1)
        sides.append(swapped(w, i, tp_count))
    side = stacked(sides)
    far = [side]
    for dy in (1, 2, 3):
        pairs = [(c, c - c % Y_COUNT + (c + dy) % Y_COUNT) for c in range(ctx_count)]
        far.append(lax.ppermute(side, "ctx", pairs))
    kept, w = (lax.dynamic_slice_in_dim(out_weight, (member ^ i) * quarter, quarter, 1) for i in (0, 1))
    paired = swapped(w, 1, tp_count)
    place = jnp.stack([member, group, y_rank])

    outs = ()
    for part in range(PARTS):
        att = attend(own, loc, core[None], queries, first, second, part, tp_count)
        atts = [att]
        for source, mask in ((0, 2), (0, 1), (1, 1)):
            atts.append(swapped(atts[source], mask, tp_count))
        atts = [atts[i] for i in (0, 2, 1, 3)]
        sent = project(place, atts, kept, paired, far)
        got = [sent[0]]
        for i in (1, 2, 3):
            got.append(swapped(sent[i], 4 * i, tp_count))
        cols = list(add_parts(member[None], got))
        for i in (1, 2, 3):
            cols[i] = swapped(cols[i], i, tp_count)
        outs = finish(member[None], static_scale, residual_in, norm_gain[None, :], cols, part, outs)
    return tuple(outs)


def solution(mesh):
    return jax.shard_map(
        shards,
        mesh=mesh,
        in_specs=(
            P("ctx", "tp"),
            P("ctx", None),
            P("ctx", None),
            P("ctx"),
            P("tp", None),
            P(("ctx", "tp"), None),
            P(),
            P(),
        ),
        out_specs=(P(("ctx", "tp"), None), P(("ctx", "tp"), None)),
        check_vma=False,
    )
```

```python
import functools
import math

import jax
import jax.numpy as jnp
from jax import lax
from jax.experimental import pallas as pl
from jax.experimental.pallas import tpu as pltpu
from jax.sharding import PartitionSpec as P


HD = 128
SPAN = 512
GW = 256
UNROLL = 2
MASKED = -1e30
LOG2_SCALE = math.log2(math.e) / math.sqrt(HD)
PARTS = 2
Y_COUNT = 4
ANY = pl.ANY
VMEM_SPEC = pl.BlockSpec(memory_space=pltpu.VMEM)


def attend_kernel(
    own_ref, loc_ref, core_ref, q_ref, first_ref, second_ref, out_ref,
    k_ref, vt_ref, qt_ref, acc_ref, max_ref, sum_ref, top_ref, factor_ref, *tile_refs,
    rows, part, heads, run,
):
    span = pl.program_id(0)
    slots = first_ref.shape[0]
    block_rows = k_ref.shape[0] // slots
    per = q_ref.shape[0] // pl.num_programs(0)
    mine = pl.ds(span * per, per)
    nrow = per * rows
    groups = nrow * heads // GW
    score_refs, weight_refs = tile_refs[:groups], tile_refs[groups:]

    @pl.when(span == 0)
    def _():
        def take(keys, values):
            for i in range(slots):
                at = i * block_rows
                k_ref[at:at + block_rows, :HD] = keys[i, :block_rows, :]
                k_ref[at:at + block_rows, HD:] = keys[i, :block_rows, :]
                for b in range(0, block_rows, SPAN):
                    vt_ref[(at + b) // SPAN] = values[i, b:b + SPAN, :].T

        @pl.when(core_ref[0] == 0)
        def _():
            take(first_ref, second_ref)

        @pl.when(core_ref[0] != 0)
        def _():
            take(second_ref, first_ref)

    own = own_ref[span]
    q_all = q_ref[mine, part * rows:(part + 1) * rows, :].reshape(nrow, heads * HD).astype(jnp.float32) * LOG2_SCALE
    for h in range(heads):
        q_t = q_all[:, h * HD:(h + 1) * HD].T
        high = q_t.astype(jnp.bfloat16)
        qt_ref[:HD, h * nrow:(h + 1) * nrow] = high
        qt_ref[HD:, h * nrow:(h + 1) * nrow] = (q_t - high.astype(jnp.float32)).astype(jnp.bfloat16)

    def score(blk, g):
        keys = k_ref[pl.ds(pl.multiple_of(blk * SPAN, SPAN), SPAN), :]
        s = jnp.dot(keys, qt_ref[:, g * GW:(g + 1) * GW], preferred_element_type=jnp.float32)
        score_refs[g][...] = s
        top_ref[g] = jnp.max(s.reshape(SPAN // 8, 8, GW), axis=0)

    def weigh(s, top, g):
        old = max_ref[g]
        new = jnp.maximum(old, jnp.broadcast_to(jnp.max(top, axis=0, keepdims=True), old.shape))
        max_ref[g] = new
        p = jnp.exp2(s.reshape(SPAN // 8, 8, GW) - new[None])
        factor = jnp.exp2(old - new)
        factor_ref[g] = factor
        sum_ref[g] = sum_ref[g] * factor + jnp.sum(p, axis=0)
        weight_refs[g][...] = p.reshape(SPAN, GW).astype(jnp.bfloat16)

    def apply(blk, g):
        pv = jnp.dot(vt_ref[blk], weight_refs[g][...], preferred_element_type=jnp.float32)
        acc_ref[g] = acc_ref[g] * factor_ref[g][None] + pv.reshape(HD // 8, 8, GW)

    max_ref[...] = jnp.full_like(max_ref, MASKED)
    sum_ref[...] = jnp.zeros_like(sum_ref)
    acc_ref[...] = jnp.zeros_like(acc_ref)
    factor_ref[...] = jnp.zeros_like(factor_ref)
    for g in range(groups):
        weight_refs[g][...] = jnp.zeros_like(weight_refs[g])
        score(loc_ref[0], g)

    def turn(t):
        prev = loc_ref[jnp.maximum(t - 1, 0)]
        for g in range(groups):
            apply(prev, g)
            weigh(score_refs[g][...], top_ref[g], g)
            score(loc_ref[t + 1], g)

    def turns(i, carry):
        for u in range(UNROLL):
            turn(i * UNROLL + u)
        return carry

    def single(t, carry):
        turn(t)
        return carry

    whole = lax.div(own, jnp.int32(UNROLL))
    lax.fori_loop(0, whole, turns, 0)
    lax.fori_loop(whole * UNROLL, own, single, 0)
    prev = loc_ref[jnp.maximum(own - 1, 0)]
    key_i = lax.broadcasted_iota(jnp.int32, (SPAN, GW), 0)
    col_i = lax.broadcasted_iota(jnp.int32, (SPAN, GW), 1)
    for g in range(groups):
        apply(prev, g)
        r = (col_i + g * GW) & (nrow - 1)
        row_i = (r >> (rows.bit_length() - 1)) * run + part * rows + (r & (rows - 1))
        s = jnp.where(key_i <= row_i, score_refs[g][...], MASKED)
        weigh(s, jnp.max(s.reshape(SPAN // 8, 8, GW), axis=0), g)
    for g in range(groups):
        apply(loc_ref[own], g)
    for g in range(groups):
        total = jnp.sum(sum_ref[g], axis=0, keepdims=True)
        done = (acc_ref[g].reshape(HD, GW) * (1.0 / total)).T.astype(jnp.bfloat16)
        n = min(nrow, GW)
        for c in range(0, GW, n):
            h, r0 = divmod(g * GW + c, nrow)
            at = pl.ds(span * per + r0 // rows, n // rows)
            out_ref[at, :, h * HD:(h + 1) * HD] = done[c:c + n].reshape(n // rows, rows, HD)


def attend(own, loc, core, queries, first, second, part, tp_count):
    tok, width = queries.shape
    heads = width // HD
    run = tok // tp_count
    rows = run // PARTS
    spans = tok // SPAN
    per = tp_count // spans
    slots = first.shape[0]
    keys = slots * tok
    groups = per * rows * heads // GW
    pairs = heads * rows * per * spans * keys
    return pl.pallas_call(
        functools.partial(attend_kernel, rows=rows, part=part, heads=heads, run=run),
        out_shape=jax.ShapeDtypeStruct((tp_count, rows, width), jnp.bfloat16),
        grid_spec=pltpu.PrefetchScalarGridSpec(
            num_scalar_prefetch=3,
            grid=(spans,),
            in_specs=[
                VMEM_SPEC,
                VMEM_SPEC,
                VMEM_SPEC,
            ],
            out_specs=VMEM_SPEC,
            scratch_shapes=[
                pltpu.VMEM((keys, 2 * HD), jnp.bfloat16),
                pltpu.VMEM((keys // SPAN, HD, SPAN), jnp.bfloat16),
                pltpu.VMEM((2 * HD, per * rows * heads), jnp.bfloat16),
                pltpu.VMEM((groups, HD // 8, 8, GW), jnp.float32),
                pltpu.VMEM((groups, 8, GW), jnp.float32),
                pltpu.VMEM((groups, 8, GW), jnp.float32),
                pltpu.VMEM((groups, 8, GW), jnp.float32),
                pltpu.VMEM((groups, 8, GW), jnp.float32),
            ]
            + [pltpu.VMEM((SPAN, GW), jnp.float32)] * groups
            + [pltpu.VMEM((SPAN, GW), jnp.bfloat16)] * groups,
        ),
        compiler_params=pltpu.CompilerParams(dimension_semantics=("arbitrary",), vmem_limit_bytes=20 * 2**20),
        cost_estimate=pl.CostEstimate(flops=8 * HD * pairs, bytes_accessed=4 * keys * HD, transcendentals=pairs),
    )(own, loc, core, queries.reshape(tp_count, run, width), first, second)


def stack_kernel(*refs):
    ins, out_ref, sems = refs[:-2], refs[-2], refs[-1]
    copies = [pltpu.make_async_copy(x, out_ref.at[i], sems.at[i]) for i, x in enumerate(ins)]
    for c in copies:
        c.start()
    for c in copies:
        c.wait()


def stacked(pieces):
    return pl.pallas_call(
        stack_kernel,
        out_shape=jax.ShapeDtypeStruct((len(pieces), *pieces[0].shape), pieces[0].dtype),
        in_specs=[pl.BlockSpec(memory_space=ANY)] * len(pieces),
        out_specs=VMEM_SPEC,
        scratch_shapes=[pltpu.SemaphoreType.DMA((len(pieces),))],
        compiler_params=pltpu.CompilerParams(vmem_limit_bytes=57 * 2**20),
    )(*pieces)


def project_kernel(place_ref, *refs):
    atts, near, far, outs, acc_ref = refs[:4], refs[4:6], refs[6:10], refs[10:14], refs[14]
    rows, cut = acc_ref.shape
    n = outs[0].shape[0]
    for j, w in enumerate(far):
        cols = pl.ds(pl.multiple_of(((place_ref[2] - j) & (len(far) - 1)) * cut, cut), cut)
        total = None
        for m, a in enumerate(atts):
            weight = near[m][:, cols] if m < 2 else w[m - 2]
            term = jnp.dot(a[...].reshape(rows, a.shape[-1]), weight, preferred_element_type=jnp.float32)
            total = term if total is None else total + term
        acc_ref[...] = total
        for i, o in enumerate(outs):
            o[:, cols] = acc_ref[pl.ds(pl.multiple_of((place_ref[1] ^ i) * n, n), n), :].astype(jnp.bfloat16)


def project(place, atts, kept, paired, far):
    tps, r, k = atts[0].shape
    rows, cut = tps * r, far[0].shape[-1]
    n = cut * len(far)
    return pl.pallas_call(
        project_kernel,
        out_shape=[jax.ShapeDtypeStruct((rows // 4, n), jnp.bfloat16)] * 4,
        in_specs=[pl.BlockSpec(memory_space=pltpu.SMEM)] + [VMEM_SPEC] * (6 + len(far)),
        out_specs=[VMEM_SPEC] * 4,
        scratch_shapes=[pltpu.VMEM((rows, cut), jnp.float32)],
        compiler_params=pltpu.CompilerParams(vmem_limit_bytes=16 * 2**20),
        cost_estimate=pl.CostEstimate(flops=8 * rows * k * n, bytes_accessed=8 * k * n, transcendentals=0),
        name="project",
    )(place, *atts, kept, paired, *far)


def add_kernel(m_ref, *refs):
    ins, outs = refs[:4], refs[4:]
    r = outs[0].shape[0]
    for i, o in enumerate(outs):
        rows = pl.ds(pl.multiple_of((m_ref[0] ^ i) * r, r), r)
        total = ins[0][rows, :].astype(jnp.float32)
        for x in ins[1:]:
            total = total + x[rows, :].astype(jnp.float32)
        o[...] = total.astype(jnp.bfloat16)


def add_parts(member, parts):
    rows, n = parts[0].shape
    return pl.pallas_call(
        add_kernel,
        out_shape=[jax.ShapeDtypeStruct((rows // 4, n), jnp.bfloat16)] * 4,
        in_specs=[pl.BlockSpec(memory_space=pltpu.SMEM)] + [VMEM_SPEC] * 4,
        out_specs=[VMEM_SPEC] * 4,
        compiler_params=pltpu.CompilerParams(vmem_limit_bytes=8 * 2**20),
        cost_estimate=pl.CostEstimate(flops=4 * rows * n, bytes_accessed=10 * rows * n, transcendentals=0),
        name="add_parts",
    )(member, *parts)


def finish_kernel(m_ref, scale_ref, res_ref, gain_ref, *refs):
    parts, (hidden_ref, clipped_ref, tmp_ref) = refs[:4], refs[4:]
    n = parts[0].shape[1]
    square = None
    for i, part in enumerate(parts):
        cols = pl.ds(pl.multiple_of((m_ref[0] ^ i) * n, n), n)
        s = res_ref[:, cols].astype(jnp.float32) + part[...].astype(jnp.float32)
        tmp_ref[:, cols] = s
        hidden_ref[:, cols] = s.astype(jnp.bfloat16)
        t = jnp.sum(s * s, axis=1, keepdims=True)
        square = t if square is None else square + t
    inv = lax.rsqrt(square / (4 * n) + 1e-05)
    limit = 448.0 * scale_ref[0]
    clipped_ref[...] = jnp.clip(tmp_ref[...] * inv * gain_ref[...], -limit, limit).astype(jnp.bfloat16)


def finish(member, static_scale, residual, gain, parts, part, before):
    rows, width = residual.shape
    r = rows // PARTS
    whole = pl.BlockSpec((r, width), lambda i, *_: (part, 0))
    kernel = finish_kernel
    if before:
        kernel = lambda m, s, res, g, a, b, c, d, e, f, *rest: finish_kernel(m, s, res, g, a, b, c, d, *rest)
    return pl.pallas_call(
        kernel,
        out_shape=[jax.ShapeDtypeStruct((rows, width), jnp.bfloat16)] * 2,
        grid_spec=pltpu.PrefetchScalarGridSpec(
            num_scalar_prefetch=2,
            grid=(1,),
            in_specs=[whole, pl.BlockSpec((1, width), lambda i, *_: (0, 0))]
            + [VMEM_SPEC] * 4
            + [pl.BlockSpec(memory_space=ANY)] * len(before),
            out_specs=[whole] * 2,
            scratch_shapes=[pltpu.VMEM((r, width), jnp.float32)],
        ),
        input_output_aliases={8 + i: i for i in range(len(before))},
        compiler_params=pltpu.CompilerParams(vmem_limit_bytes=12 * 2**20),
        cost_estimate=pl.CostEstimate(flops=8 * r * width, bytes_accessed=10 * r * width, transcendentals=0),
    )(member, static_scale, residual, gain, *parts, *before)


def swapped(value, mask, count):
    return lax.ppermute(value, "tp", [(i, i ^ mask) for i in range(count)])


def shards(
    queries,
    context_keys,
    context_values,
    positions,
    out_weight,
    residual_in,
    norm_gain,
    static_scale,
):
    ctx_count = lax.axis_size("ctx")
    tp_count = lax.axis_size("tp")
    tp_rank = lax.axis_index("tp").astype(jnp.int32)
    tok, _ = queries.shape
    core = tp_rank & 1
    member = tp_rank & 3
    group = tp_rank >> 2
    y_rank = lax.axis_index("ctx").astype(jnp.int32) & (Y_COUNT - 1)

    kv_col = (tp_rank >> 1) * HD
    mine = jnp.where(
        core == 0,
        lax.dynamic_slice_in_dim(context_keys, kv_col, HD, 1),
        lax.dynamic_slice_in_dim(context_values, kv_col, HD, 1),
    )
    spans = tok // SPAN
    own = positions[::SPAN] // SPAN
    tag = jnp.pad(own.astype(jnp.bfloat16)[:, None] * jnp.ones((1, HD), jnp.bfloat16), ((0, 16 - spans), (0, 0)))
    mine = jnp.concatenate([mine, tag], axis=0)
    pieces = [mine]
    for dz in range(ctx_count // Y_COUNT):
        for dy in (0, 2, 1, 3):
            if dz or dy:
                pairs = [
                    (c, (c // Y_COUNT ^ dz) * Y_COUNT + (c + dy) % Y_COUNT) for c in range(ctx_count)
                ]
                pieces.append(lax.ppermute(mine, "ctx", pairs))
    first = stacked(pieces)
    second = swapped(first, 1, tp_count)
    order = first[:, tok:tok + spans, 0].reshape(ctx_count * spans).astype(jnp.int32)
    blocks = jnp.arange(ctx_count * spans, dtype=jnp.int32)
    loc = jnp.sum(jnp.where(order[None, :] == blocks[:, None], blocks[None, :], 0), axis=1)

    quarter = out_weight.shape[1] // 4
    cut = quarter // Y_COUNT
    sides = []
    for i in (2, 3):
        w = lax.dynamic_slice_in_dim(out_weight, (member ^ i) * quarter + y_rank * cut, cut, 1)
        sides.append(swapped(w, i, tp_count))
    side = stacked(sides)
    far = [side]
    for dy in (1, 2, 3):
        pairs = [(c, c - c % Y_COUNT + (c + dy) % Y_COUNT) for c in range(ctx_count)]
        far.append(lax.ppermute(side, "ctx", pairs))
    kept, w = (lax.dynamic_slice_in_dim(out_weight, (member ^ i) * quarter, quarter, 1) for i in (0, 1))
    paired = swapped(w, 1, tp_count)
    place = jnp.stack([member, group, y_rank])

    outs = ()
    for part in range(PARTS):
        att = attend(own, loc, core[None], queries, first, second, part, tp_count)
        atts = [att]
        routes = ((0, 2), (0, 1), (0, 3) if part == 0 else (1, 1))
        for source, mask in routes:
            atts.append(swapped(atts[source], mask, tp_count))
        atts = [atts[i] for i in (0, 2, 1, 3)]
        sent = project(place, atts, kept, paired, far)
        got = [sent[0]]
        for i in (1, 2, 3):
            got.append(swapped(sent[i], 4 * i, tp_count))
        cols = list(add_parts(member[None], got))
        for i in (1, 2, 3):
            cols[i] = swapped(cols[i], i, tp_count)
        outs = finish(member[None], static_scale, residual_in, norm_gain[None, :], cols, part, outs)
    return tuple(outs)


def solution(mesh):
    return jax.shard_map(
        shards,
        mesh=mesh,
        in_specs=(
            P("ctx", "tp"),
            P("ctx", None),
            P("ctx", None),
            P("ctx"),
            P("tp", None),
            P(("ctx", "tp"), None),
            P(),
            P(),
        ),
        out_specs=(P(("ctx", "tp"), None), P(("ctx", "tp"), None)),
        check_vma=False,
    )
```

```python
import functools
import math

import jax
import jax.numpy as jnp
from jax import lax
from jax.experimental import pallas as pl
from jax.experimental.pallas import tpu as pltpu
from jax.sharding import PartitionSpec as P


HD = 128
SPAN = 512
GW = 256
UNROLL = 2
MASKED = -1e30
LOG2_SCALE = math.log2(math.e) / math.sqrt(HD)
PARTS = 2
Y_COUNT = 4
ANY = pl.ANY
VMEM_SPEC = pl.BlockSpec(memory_space=pltpu.VMEM)


def attend_kernel(
    own_ref, loc_ref, core_ref, q_ref, first_ref, second_ref, out_ref,
    k_ref, vt_ref, qt_ref, acc_ref, max_ref, sum_ref, top_ref, factor_ref, *tile_refs,
    rows, part, heads, run,
):
    span = pl.program_id(0)
    slots = first_ref.shape[0]
    block_rows = k_ref.shape[0] // slots
    per = q_ref.shape[0] // pl.num_programs(0)
    mine = pl.ds(span * per, per)
    nrow = per * rows
    groups = nrow * heads // GW
    score_refs, weight_refs = tile_refs[:groups], tile_refs[groups:]

    @pl.when(span == 0)
    def _():
        def take(keys, values):
            for i in range(slots):
                at = i * block_rows
                k_ref[at:at + block_rows, :HD] = keys[i, :block_rows, :]
                k_ref[at:at + block_rows, HD:] = keys[i, :block_rows, :]
                for b in range(0, block_rows, SPAN):
                    vt_ref[(at + b) // SPAN] = values[i, b:b + SPAN, :].T

        @pl.when(core_ref[0] == 0)
        def _():
            take(first_ref, second_ref)

        @pl.when(core_ref[0] != 0)
        def _():
            take(second_ref, first_ref)

    own = own_ref[span]
    q_all = q_ref[mine, part * rows:(part + 1) * rows, :].reshape(nrow, heads * HD).astype(jnp.float32) * LOG2_SCALE
    for h in range(heads):
        q_t = q_all[:, h * HD:(h + 1) * HD].T
        high = q_t.astype(jnp.bfloat16)
        qt_ref[:HD, h * nrow:(h + 1) * nrow] = high
        qt_ref[HD:, h * nrow:(h + 1) * nrow] = (q_t - high.astype(jnp.float32)).astype(jnp.bfloat16)

    def score(blk, g):
        keys = k_ref[pl.ds(pl.multiple_of(blk * SPAN, SPAN), SPAN), :]
        s = jnp.dot(keys, qt_ref[:, g * GW:(g + 1) * GW], preferred_element_type=jnp.float32)
        score_refs[g][...] = s
        top_ref[g] = jnp.max(s.reshape(SPAN // 8, 8, GW), axis=0)

    def weigh(s, top, g):
        old = max_ref[g]
        new = jnp.maximum(old, jnp.broadcast_to(jnp.max(top, axis=0, keepdims=True), old.shape))
        max_ref[g] = new
        p = jnp.exp2(s.reshape(SPAN // 8, 8, GW) - new[None])
        factor = jnp.exp2(old - new)
        factor_ref[g] = factor
        sum_ref[g] = sum_ref[g] * factor + jnp.sum(p, axis=0)
        weight_refs[g][...] = p.reshape(SPAN, GW).astype(jnp.bfloat16)

    def apply(blk, g):
        pv = jnp.dot(vt_ref[blk], weight_refs[g][...], preferred_element_type=jnp.float32)
        acc_ref[g] = acc_ref[g] * factor_ref[g][None] + pv.reshape(HD // 8, 8, GW)

    max_ref[...] = jnp.full_like(max_ref, MASKED)
    sum_ref[...] = jnp.zeros_like(sum_ref)
    acc_ref[...] = jnp.zeros_like(acc_ref)
    factor_ref[...] = jnp.zeros_like(factor_ref)
    for g in range(groups):
        weight_refs[g][...] = jnp.zeros_like(weight_refs[g])
        score(loc_ref[0], g)

    def turn(t):
        prev = loc_ref[jnp.maximum(t - 1, 0)]
        for g in range(groups):
            apply(prev, g)
            weigh(score_refs[g][...], top_ref[g], g)
            score(loc_ref[t + 1], g)

    def turns(i, carry):
        for u in range(UNROLL):
            turn(i * UNROLL + u)
        return carry

    def single(t, carry):
        turn(t)
        return carry

    whole = lax.div(own, jnp.int32(UNROLL))
    lax.fori_loop(0, whole, turns, 0)
    lax.fori_loop(whole * UNROLL, own, single, 0)
    prev = loc_ref[jnp.maximum(own - 1, 0)]
    key_i = lax.broadcasted_iota(jnp.int32, (SPAN, GW), 0)
    col_i = lax.broadcasted_iota(jnp.int32, (SPAN, GW), 1)
    for g in range(groups):
        apply(prev, g)
        r = (col_i + g * GW) & (nrow - 1)
        row_i = (r >> (rows.bit_length() - 1)) * run + part * rows + (r & (rows - 1))
        s = jnp.where(key_i <= row_i, score_refs[g][...], MASKED)
        weigh(s, jnp.max(s.reshape(SPAN // 8, 8, GW), axis=0), g)
    for g in range(groups):
        apply(loc_ref[own], g)
    for g in range(groups):
        total = jnp.sum(sum_ref[g], axis=0, keepdims=True)
        done = (acc_ref[g].reshape(HD, GW) * (1.0 / total)).T.astype(jnp.bfloat16)
        n = min(nrow, GW)
        for c in range(0, GW, n):
            h, r0 = divmod(g * GW + c, nrow)
            at = pl.ds(span * per + r0 // rows, n // rows)
            out_ref[at, :, h * HD:(h + 1) * HD] = done[c:c + n].reshape(n // rows, rows, HD)


def attend(own, loc, core, queries, first, second, part, tp_count):
    tok, width = queries.shape
    heads = width // HD
    run = tok // tp_count
    rows = run // PARTS
    spans = tok // SPAN
    per = tp_count // spans
    slots = first.shape[0]
    keys = slots * tok
    groups = per * rows * heads // GW
    pairs = heads * rows * per * spans * keys
    return pl.pallas_call(
        functools.partial(attend_kernel, rows=rows, part=part, heads=heads, run=run),
        out_shape=jax.ShapeDtypeStruct((tp_count, rows, width), jnp.bfloat16),
        grid_spec=pltpu.PrefetchScalarGridSpec(
            num_scalar_prefetch=3,
            grid=(spans,),
            in_specs=[
                VMEM_SPEC,
                VMEM_SPEC,
                VMEM_SPEC,
            ],
            out_specs=VMEM_SPEC,
            scratch_shapes=[
                pltpu.VMEM((keys, 2 * HD), jnp.bfloat16),
                pltpu.VMEM((keys // SPAN, HD, SPAN), jnp.bfloat16),
                pltpu.VMEM((2 * HD, per * rows * heads), jnp.bfloat16),
                pltpu.VMEM((groups, HD // 8, 8, GW), jnp.float32),
                pltpu.VMEM((groups, 8, GW), jnp.float32),
                pltpu.VMEM((groups, 8, GW), jnp.float32),
                pltpu.VMEM((groups, 8, GW), jnp.float32),
                pltpu.VMEM((groups, 8, GW), jnp.float32),
            ]
            + [pltpu.VMEM((SPAN, GW), jnp.float32)] * groups
            + [pltpu.VMEM((SPAN, GW), jnp.bfloat16)] * groups,
        ),
        compiler_params=pltpu.CompilerParams(dimension_semantics=("arbitrary",), vmem_limit_bytes=20 * 2**20),
        cost_estimate=pl.CostEstimate(flops=8 * HD * pairs, bytes_accessed=4 * keys * HD, transcendentals=pairs),
    )(own, loc, core, queries.reshape(tp_count, run, width), first, second)


def stack_kernel(*refs):
    ins, out_ref, sems = refs[:-2], refs[-2], refs[-1]
    copies = [pltpu.make_async_copy(x, out_ref.at[i], sems.at[i]) for i, x in enumerate(ins)]
    for c in copies:
        c.start()
    for c in copies:
        c.wait()


def stacked(pieces):
    return pl.pallas_call(
        stack_kernel,
        out_shape=jax.ShapeDtypeStruct((len(pieces), *pieces[0].shape), pieces[0].dtype),
        in_specs=[pl.BlockSpec(memory_space=ANY)] * len(pieces),
        out_specs=VMEM_SPEC,
        scratch_shapes=[pltpu.SemaphoreType.DMA((len(pieces),))],
        compiler_params=pltpu.CompilerParams(vmem_limit_bytes=57 * 2**20),
    )(*pieces)


def project_kernel(place_ref, *refs):
    atts, near, across, far, outs, acc_ref = refs[:4], refs[4:6], refs[6:8], refs[8:12], refs[12:16], refs[16]
    rows = acc_ref.shape[0]
    n = outs[0].shape[0]
    direct, cut = across[0].shape[1], far[0].shape[2]

    def multiply(cols, width, others):
        total = None
        for a, weight in zip(atts, [w[:, cols] for w in near] + others):
            term = jnp.dot(a[...].reshape(rows, a.shape[-1]), weight, preferred_element_type=jnp.float32)
            total = term if total is None else total + term
        acc_ref[:, :width] = total
        for i, o in enumerate(outs):
            group = pl.ds(pl.multiple_of((place_ref[1] ^ i) * n, n), n)
            o[:, cols] = acc_ref[group, :width].astype(jnp.bfloat16)

    wide = acc_ref.shape[1]
    for c in range(0, direct, wide):
        multiply(slice(c, c + wide), wide, [w[:, c:c + wide] for w in across])
    for j, w in enumerate(far):
        at = direct + ((place_ref[2] - j) & (len(far) - 1)) * cut
        multiply(pl.ds(pl.multiple_of(at, cut), cut), cut, [w[0], w[1]])


def project(place, atts, near, across, far):
    tps, r, k = atts[0].shape
    rows, n = tps * r, near[0].shape[1]
    return pl.pallas_call(
        project_kernel,
        out_shape=[jax.ShapeDtypeStruct((rows // 4, n), jnp.bfloat16)] * 4,
        in_specs=[pl.BlockSpec(memory_space=pltpu.SMEM)] + [VMEM_SPEC] * (8 + len(far)),
        out_specs=[VMEM_SPEC] * 4,
        scratch_shapes=[pltpu.VMEM((rows, across[0].shape[1] // 2), jnp.float32)],
        compiler_params=pltpu.CompilerParams(vmem_limit_bytes=16 * 2**20),
        cost_estimate=pl.CostEstimate(flops=8 * rows * k * n, bytes_accessed=8 * k * n, transcendentals=0),
        name="project",
    )(place, *atts, *near, *across, *far)


def add_kernel(m_ref, *refs):
    ins, outs = refs[:4], refs[4:]
    r = outs[0].shape[0]
    for i, o in enumerate(outs):
        rows = pl.ds(pl.multiple_of((m_ref[0] ^ i) * r, r), r)
        total = ins[0][rows, :].astype(jnp.float32)
        for x in ins[1:]:
            total = total + x[rows, :].astype(jnp.float32)
        o[...] = total.astype(jnp.bfloat16)


def add_parts(member, parts):
    rows, n = parts[0].shape
    return pl.pallas_call(
        add_kernel,
        out_shape=[jax.ShapeDtypeStruct((rows // 4, n), jnp.bfloat16)] * 4,
        in_specs=[pl.BlockSpec(memory_space=pltpu.SMEM)] + [VMEM_SPEC] * 4,
        out_specs=[VMEM_SPEC] * 4,
        compiler_params=pltpu.CompilerParams(vmem_limit_bytes=8 * 2**20),
        cost_estimate=pl.CostEstimate(flops=4 * rows * n, bytes_accessed=10 * rows * n, transcendentals=0),
        name="add_parts",
    )(member, *parts)


def finish_kernel(m_ref, scale_ref, res_ref, gain_ref, *refs):
    parts, (hidden_ref, clipped_ref, tmp_ref) = refs[:4], refs[4:]
    n = parts[0].shape[1]
    square = None
    for i, part in enumerate(parts):
        cols = pl.ds(pl.multiple_of((m_ref[0] ^ i) * n, n), n)
        s = res_ref[:, cols].astype(jnp.float32) + part[...].astype(jnp.float32)
        tmp_ref[:, cols] = s
        hidden_ref[:, cols] = s.astype(jnp.bfloat16)
        t = jnp.sum(s * s, axis=1, keepdims=True)
        square = t if square is None else square + t
    inv = lax.rsqrt(square / (4 * n) + 1e-05)
    limit = 448.0 * scale_ref[0]
    clipped_ref[...] = jnp.clip(tmp_ref[...] * inv * gain_ref[...], -limit, limit).astype(jnp.bfloat16)


def finish(member, static_scale, residual, gain, parts, part, before):
    rows, width = residual.shape
    r = rows // PARTS
    whole = pl.BlockSpec((r, width), lambda i, *_: (part, 0))
    kernel = finish_kernel
    if before:
        kernel = lambda m, s, res, g, a, b, c, d, e, f, *rest: finish_kernel(m, s, res, g, a, b, c, d, *rest)
    return pl.pallas_call(
        kernel,
        out_shape=[jax.ShapeDtypeStruct((rows, width), jnp.bfloat16)] * 2,
        grid_spec=pltpu.PrefetchScalarGridSpec(
            num_scalar_prefetch=2,
            grid=(1,),
            in_specs=[whole, pl.BlockSpec((1, width), lambda i, *_: (0, 0))]
            + [VMEM_SPEC] * 4
            + [pl.BlockSpec(memory_space=ANY)] * len(before),
            out_specs=[whole] * 2,
            scratch_shapes=[pltpu.VMEM((r, width), jnp.float32)],
        ),
        input_output_aliases={8 + i: i for i in range(len(before))},
        compiler_params=pltpu.CompilerParams(vmem_limit_bytes=12 * 2**20),
        cost_estimate=pl.CostEstimate(flops=8 * r * width, bytes_accessed=10 * r * width, transcendentals=0),
    )(member, static_scale, residual, gain, *parts, *before)


def swapped(value, mask, count):
    return lax.ppermute(value, "tp", [(i, i ^ mask) for i in range(count)])


def shards(
    queries,
    context_keys,
    context_values,
    positions,
    out_weight,
    residual_in,
    norm_gain,
    static_scale,
):
    ctx_count = lax.axis_size("ctx")
    tp_count = lax.axis_size("tp")
    tp_rank = lax.axis_index("tp").astype(jnp.int32)
    tok, _ = queries.shape
    core = tp_rank & 1
    member = tp_rank & 3
    group = tp_rank >> 2
    y_rank = lax.axis_index("ctx").astype(jnp.int32) & (Y_COUNT - 1)

    kv_col = (tp_rank >> 1) * HD
    mine = jnp.where(
        core == 0,
        lax.dynamic_slice_in_dim(context_keys, kv_col, HD, 1),
        lax.dynamic_slice_in_dim(context_values, kv_col, HD, 1),
    )
    spans = tok // SPAN
    own = positions[::SPAN] // SPAN
    tag = jnp.pad(own.astype(jnp.bfloat16)[:, None] * jnp.ones((1, HD), jnp.bfloat16), ((0, 16 - spans), (0, 0)))
    mine = jnp.concatenate([mine, tag], axis=0)
    pieces = [mine]
    for dz in range(ctx_count // Y_COUNT):
        for dy in (0, 2, 1, 3):
            if dz or dy:
                pairs = [
                    (c, (c // Y_COUNT ^ dz) * Y_COUNT + (c + dy) % Y_COUNT) for c in range(ctx_count)
                ]
                pieces.append(lax.ppermute(mine, "ctx", pairs))
    first = stacked(pieces)
    second = swapped(first, 1, tp_count)
    order = first[:, tok:tok + spans, 0].reshape(ctx_count * spans).astype(jnp.int32)
    blocks = jnp.arange(ctx_count * spans, dtype=jnp.int32)
    loc = jnp.sum(jnp.where(order[None, :] == blocks[:, None], blocks[None, :], 0), axis=1)

    quarter = out_weight.shape[1] // 4
    direct = quarter // 2
    cut = (quarter - direct) // Y_COUNT
    sides = []
    for i in (2, 3):
        w = lax.dynamic_slice_in_dim(out_weight, (member ^ i) * quarter + direct + y_rank * cut, cut, 1)
        sides.append(swapped(w, i, tp_count))
    side = stacked(sides)
    far = [side]
    for dy in (1, 2, 3):
        pairs = [(c, c - c % Y_COUNT + (c + dy) % Y_COUNT) for c in range(ctx_count)]
        far.append(lax.ppermute(side, "ctx", pairs))
    across = []
    for i in (2, 3):
        w = lax.dynamic_slice_in_dim(out_weight, (member ^ i) * quarter, direct, 1)
        across.append(swapped(w, i, tp_count))
    kept, w = (lax.dynamic_slice_in_dim(out_weight, (member ^ i) * quarter, quarter, 1) for i in (0, 1))
    paired = swapped(w, 1, tp_count)
    place = jnp.stack([member, group, y_rank])

    outs = ()
    for part in range(PARTS):
        att = attend(own, loc, core[None], queries, first, second, part, tp_count)
        atts = [att]
        routes = ((0, 2), (0, 1), (1, 1))
        for source, mask in routes:
            atts.append(swapped(atts[source], mask, tp_count))
        atts = [atts[i] for i in (0, 2, 1, 3)]
        sent = project(place, atts, (kept, paired), across, far)
        got = [sent[0]]
        for i in (1, 2, 3):
            got.append(swapped(sent[i], 4 * i, tp_count))
        cols = list(add_parts(member[None], got))
        for i in (1, 2, 3):
            cols[i] = swapped(cols[i], i, tp_count)
        outs = finish(member[None], static_scale, residual_in, norm_gain[None, :], cols, part, outs)
    return tuple(outs)


def solution(mesh):
    return jax.shard_map(
        shards,
        mesh=mesh,
        in_specs=(
            P("ctx", "tp"),
            P("ctx", None),
            P("ctx", None),
            P("ctx"),
            P("tp", None),
            P(("ctx", "tp"), None),
            P(),
            P(),
        ),
        out_specs=(P(("ctx", "tp"), None), P(("ctx", "tp"), None)),
        check_vma=False,
    )
```
